256 devices in a mesh: gx: 8 (over x, z_lo), gy: 4 (over y), gz: 8 (over z_hi, core).
Axes of the slice: x: 4, y: 4, z: 8 (z_hi: 4, z_lo: 2; z = z_hi * 2 + z_lo), core: 2. Of those that a mesh axis runs over, the one named last changes fastest.
Arguments:
- positions: float32 [3, 262144], P(None, ('gx', 'gy', 'gz')), may hold values from 0 to 32, as said below
- velocities: float32 [3, 262144], P(None, ('gx', 'gy', 'gz')), may hold values from -6 to 6
- inv_mass: float32 [262144], P(('gx', 'gy', 'gz')), may hold values from 0.5 to 2
- charge: float32 [262144], P(('gx', 'gy', 'gz')), may hold values from -4 to 4
- fast_force: float32 [3, 262144], P(None, ('gx', 'gy', 'gz')), may hold values from -6 to 6
- slow_force: float32 [3, 262144], P(None, ('gx', 'gy', 'gz')), may hold values from -6 to 6
- bonds: int32 [2, 262144], P(None, ('gx', 'gy', 'gz')), may hold values from 0 to 1023
- bond_k: float32 [262144], P(('gx', 'gy', 'gz')), may hold values from 0.05 to 0.4
- halo_index: int32 [6, 65536], P(None, ('gx', 'gy', 'gz')), may hold values from 0 to 1023
- pair_own: int32 [49152], P(('gx', 'gy', 'gz')), may hold values from 0 to 7
- pair_partner: int32 [49152], P(('gx', 'gy', 'gz')), may hold values from 0 to 19
- pair_count: int32 [256], P(('gx', 'gy', 'gz')), may hold values from 1 to 192
Outputs:
- displacement: float32 [3, 262144], P(None, ('gx', 'gy', 'gz'))
- velocities_out: float32 [3, 262144], P(None, ('gx', 'gy', 'gz'))
- fast_out: float32 [3, 262144], P(None, ('gx', 'gy', 'gz'))
- slow_out: float32 [3, 262144], P(None, ('gx', 'gy', 'gz'))
The draws below stay inside these ranges and needn't reach their ends.
Inputs may be any that keep to these rules, and one draw needn't show every extreme that they name: `positions`: atoms of patch p lie in the cube of side 4 at 4 times its grid place.
All inputs are finite; a program needn't handle non-finite values.
Results may differ from the reference program's by a relative error of at most 0.0003.
Values sent between devices are 32-bit elements; how exact they have to be, the bound alone decides.
A program may use at most 64 MiB of HBM per device.

```python
import math
import jax
import jax.numpy as jnp
from jax import lax

ATOMS_DEV = 1024
HALO = 256
INNER = 4
PER_PEER = 6
ATOMS = 262144
TILES_DEV = 8
PARTNERS = 20
PAIR_SLOTS = 192
NBONDS = 1024
N_GX = 8
N_GY = 4
N_GZ = 8
DEVICES = 256


patch_side = 4.0


face_margin = 1.0


def face_slots(key):
    patches = N_GX * N_GY * N_GZ
    return jax.random.randint(jax.random.fold_in(key, 11), (6, patches * HALO), 0, ATOMS_DEV).astype(jnp.int32)


def draw_halo_index(key, part):
    return face_slots(key)


def draw_positions(key, part):
    patches = N_GX * N_GY * N_GZ
    inside = jax.random.uniform(jax.random.fold_in(key, 3), (3, patches, ATOMS_DEV), jnp.float32, 0.0, patch_side)
    depth = jax.random.uniform(jax.random.fold_in(key, 5), (6, patches, HALO), jnp.float32, 0.0, face_margin)
    slots = face_slots(key).reshape(6, patches, HALO)
    patch_rows = jnp.arange(patches)[:, None]
    for face_id in range(6):
        axis_id = face_id // 2
        if face_id % 2 == 0:
            placed = depth[face_id]
        else:
            placed = patch_side - depth[face_id]
        inside = inside.at[axis_id, patch_rows, slots[face_id]].set(placed)
    patch_ids = jnp.arange(patches)
    anchor = jnp.stack([patch_ids // (N_GY * N_GZ), patch_ids // N_GZ % N_GY, patch_ids % N_GZ]).astype(jnp.float32)
    return (inside + patch_side * anchor[:, :, None]).reshape(3, patches * ATOMS_DEV)


def with_ends(drawn, stream_key, smallest, top_value):
    extent = drawn.shape
    index_at = [jax.random.randint(jax.random.fold_in(stream_key, axis), (), 0, extent[axis]) for axis in range(len(extent))]
    drawn = drawn.at[tuple(index_at)].set(smallest)
    longest = extent.index(max(extent))
    index_at[longest] = (index_at[longest] + 1) % extent[longest]
    return drawn.at[tuple(index_at)].set(top_value)


def steps_of(rng, extent, split, least, top_value):
    def one(position, blocks):
        draws = jax.random.uniform(jax.random.fold_in(jax.random.fold_in(rng, 6), position), (blocks,), jnp.float32, least / len(split), top_value / len(split))
        return jnp.repeat(jnp.exp(draws), extent[position] // blocks).reshape((-1,) + (1,) * (len(extent) - position - 1))

    gain = one(*split[0])
    for cut in split[1:]:
        gain = gain * one(*cut)
    return gain


def normal_values(key, shape, width, reach, cuts=(), dtype=jnp.bfloat16):
    entries = jax.random.normal(key, shape, jnp.float32) * width
    if len(cuts) > 0:
        entries = steps_of(key, shape, cuts, -0.22, 0.18) * entries
    return jnp.clip(entries, min=-reach, max=reach).astype(dtype)


def setup_inputs(seed: int = 0) -> dict:
    seeds = jax.random.split(jax.random.key(seed), 13)
    return {
        "positions": draw_positions(jax.random.fold_in(seeds[12], 71), 0),
        "velocities": normal_values(seeds[1], (3, ATOMS), 1.0, 6.0, ((1, 256),), jnp.float32),
        "inv_mass": jnp.clip(jnp.exp(math.log(2.0) - 1.3862944 * jax.random.uniform(seeds[2], (ATOMS,), jnp.float32) ** steps_of(seeds[2], (ATOMS,), ((0, 256),), -0.2, 0.2)), 0.5, 2.0),
        "charge": normal_values(seeds[3], (ATOMS,), 1.0, 4.0, ((0, 256),), jnp.float32),
        "fast_force": normal_values(seeds[4], (3, ATOMS), 1.0, 6.0, ((1, 256),), jnp.float32),
        "slow_force": normal_values(seeds[5], (3, ATOMS), 1.0, 6.0, ((1, 256),), jnp.float32),
        "bonds": with_ends(jax.random.randint(seeds[6], (2, NBONDS * DEVICES), 0, ATOMS_DEV), jax.random.fold_in(seeds[6], 1), 0, ATOMS_DEV - 1).astype(jnp.int32),
        "bond_k": jnp.clip(jnp.exp(math.log(0.4) - 2.0794415 * jax.random.uniform(seeds[7], (NBONDS * DEVICES,), jnp.float32) ** steps_of(seeds[7], (NBONDS * DEVICES,), ((0, 256),), -0.2, 0.2)), 0.05, 0.4),
        "halo_index": draw_halo_index(jax.random.fold_in(seeds[12], 71), 0),
        "pair_own": with_ends(jax.random.randint(seeds[9], (PAIR_SLOTS * DEVICES,), 0, TILES_DEV), jax.random.fold_in(seeds[9], 1), 0, TILES_DEV - 1).astype(jnp.int32),
        "pair_partner": with_ends(jax.random.randint(seeds[10], (PAIR_SLOTS * DEVICES,), 0, PARTNERS), jax.random.fold_in(seeds[10], 1), 0, PARTNERS - 1).astype(jnp.int32),
        "pair_count": with_ends(jax.random.randint(seeds[11], (DEVICES,), 1, PAIR_SLOTS + 1), jax.random.fold_in(seeds[11], 1), 1, PAIR_SLOTS).astype(jnp.int32),
    }


step_inner = 0.1
short_scale = 1.0
short_reach = 0.64
long_scale = 0.5
long_reach = 1.44


def short_block(row_piece, others, weight):
    separation = row_piece[:, :, None] - others[:, None, :]
    nearness = jnp.maximum(1.0 - jnp.sum(separation * separation, axis=0) / short_reach, 0.0) * weight[None, :]
    return short_scale * jnp.sum(separation * nearness[None], axis=2)


def short_force(own, others, weight):
    row_count = own.shape[1]
    block_rows = min(512, row_count)
    pieces = own.reshape(3, row_count // block_rows, block_rows).transpose(1, 0, 2)
    result = lax.map(lambda row_piece: short_block(row_piece, others, weight), pieces)
    return result.transpose(1, 0, 2).reshape(3, row_count)


def tile_force(packet):
    separation = packet[0:3, :, None] - packet[4:7, None, :]
    nearness = jnp.maximum(1.0 - jnp.sum(separation * separation, axis=0) / long_reach, 0.0) * packet[7][None, :]
    return long_scale * packet[3][None, :] * jnp.sum(separation * nearness[None], axis=2)


def block_forces(packets):
    return lax.map(lambda source_group: jax.vmap(tile_force)(source_group), packets)


def from_lower(block_data, dimension):
    edge = jnp.zeros_like(lax.slice_in_dim(block_data, 0, 1, axis=dimension))
    kept = lax.slice_in_dim(block_data, 0, block_data.shape[dimension] - 1, axis=dimension)
    return jnp.concatenate([edge, kept], axis=dimension)


def from_upper(block_data, dimension):
    edge = jnp.zeros_like(lax.slice_in_dim(block_data, 0, 1, axis=dimension))
    kept = lax.slice_in_dim(block_data, 1, block_data.shape[dimension], axis=dimension)
    return jnp.concatenate([kept, edge], axis=dimension)


def bonded_all(current, bonds, bond_k):
    offsets = ((jnp.arange(bonds.shape[1]) // ATOMS_DEV) * ATOMS_DEV).astype(jnp.int32)
    first = bonds[0].astype(jnp.int32) + offsets
    second = bonds[1].astype(jnp.int32) + offsets
    bond_pull = bond_k[None, :] * (current[:, first] - current[:, second])
    zero_force = jnp.zeros_like(current)
    return zero_force.at[:, first].add(-bond_pull).at[:, second].add(bond_pull)


def fast_all(current, charge, bonds, bond_k, halo_index):
    patches = N_GX * N_GY * N_GZ
    stacked = jnp.concatenate([current, charge[None, :]], axis=0)
    grid = stacked.reshape(4, N_GX, N_GY, N_GZ, ATOMS_DEV)
    index_grid = halo_index.reshape(6, N_GX, N_GY, N_GZ, HALO)
    faces = []
    for face_id in range(6):
        wide_index = jnp.broadcast_to(index_grid[face_id][None], (4, N_GX, N_GY, N_GZ, HALO))
        faces.append(jnp.take_along_axis(grid, wide_index, axis=4))
    unit = jnp.ones((1, N_GX, N_GY, N_GZ, HALO), jnp.float32)
    pieces = [grid]
    marks = [jnp.ones((1, N_GX, N_GY, N_GZ, ATOMS_DEV), jnp.float32)]
    for axis_id in range(3):
        dimension = axis_id + 1
        pieces.append(from_lower(faces[2 * axis_id + 1], dimension))
        pieces.append(from_upper(faces[2 * axis_id], dimension))
        marks.append(from_lower(unit, dimension))
        marks.append(from_upper(unit, dimension))
    others = jnp.concatenate(pieces, axis=4).reshape(4, patches, -1).transpose(1, 0, 2)
    weight = jnp.concatenate(marks, axis=4).reshape(patches, -1)
    own = current.reshape(3, patches, ATOMS_DEV).transpose(1, 0, 2)
    short = lax.map(lambda item: short_force(item[0], item[1][:3], item[2]), (own, others, weight))
    short = short.transpose(1, 0, 2).reshape(3, -1)
    return short + bonded_all(current, bonds, bond_k), stacked, others


def slow_all(stacked, others, pair_own, pair_partner, pair_count):
    patches = N_GX * N_GY * N_GZ
    slot_count = pair_own.shape[0] // patches
    tile_count = ATOMS_DEV // 128
    own_tiles = stacked.reshape(4, patches, tile_count, 128).transpose(1, 2, 0, 3)
    partners = others.reshape(patches, 4, -1, 128).transpose(0, 2, 1, 3)
    own_index = pair_own.reshape(patches, slot_count).astype(jnp.int32)
    partner_index = pair_partner.reshape(patches, slot_count).astype(jnp.int32)
    own_rows = jax.vmap(lambda tiles_of, chosen: tiles_of[chosen])(own_tiles, own_index)
    partner_rows = jax.vmap(lambda tiles_of, chosen: tiles_of[chosen])(partners, partner_index)
    live_slots = (jnp.arange(slot_count)[None, :] < pair_count[:, None]).astype(jnp.float32)
    packets = jnp.concatenate([own_rows[:, :, :3], own_rows[:, :, 3:] * live_slots[:, :, None, None], partner_rows], axis=2)
    tile_terms = lax.map(lambda patch_packets: block_forces(patch_packets.reshape(-1, PER_PEER, 8, 128)).reshape(-1, 3, 128), packets)
    select = (own_index[:, :, None] == jnp.arange(tile_count)[None, None, :]).astype(jnp.float32)
    slow_now = jnp.einsum("pst,psck->cptk", select, tile_terms, precision=lax.Precision.HIGHEST)
    return slow_now.reshape(3, -1)


def reference(positions, velocities, inv_mass, charge, fast_force, slow_force, bonds, bond_k, halo_index, pair_own, pair_partner, pair_count):
    half_inner = 0.5 * step_inner
    half_outer = 0.5 * INNER * step_inner
    moving = velocities + half_outer * inv_mass[None, :] * slow_force
    current = positions
    force_now = fast_force
    for inner_turn in range(INNER):
        moving = moving + half_inner * inv_mass[None, :] * force_now
        current = current + step_inner * moving
        force_now, stacked, others = fast_all(current, charge, bonds, bond_k, halo_index)
        moving = moving + half_inner * inv_mass[None, :] * force_now
    slow_now = slow_all(stacked, others, pair_own, pair_partner, pair_count)
    moving = moving + half_outer * inv_mass[None, :] * slow_now
    return current - positions, moving, force_now, slow_now
```

```python
import functools

import jax
import jax.numpy as jnp
from jax import lax
from jax.experimental import pallas as pl
from jax.experimental.pallas import tpu as pltpu
from jax.sharding import PartitionSpec as P

MESH = pl.DeviceIdType.MESH
F32 = jnp.float32
BF16 = jnp.bfloat16

INNER = 4
STEP = 0.1
SIDE = 4.0
SHORT_SCALE = 1.0
SHORT_INV = 1.0 / 0.64
LONG_SCALE = 0.5
LONG_INV = 1.0 / 1.44
FAR = 1e30

ATOMS = 1024
HALO = 256
FACES = 6
VISIBLE = ATOMS + FACES * HALO
BLOCK = 256
KDIM = 48
TILE = 128
OWN_TILES = ATOMS // TILE
SLOTS = 192
AXES = ("gx", "gy", "gz")


def rows_like(shape):
    return lax.broadcasted_iota(jnp.int32, shape, 0)


def lanes_like(shape):
    return lax.broadcasted_iota(jnp.int32, shape, 1)


def split3(a):
    high = a.astype(BF16).astype(F32)
    rest = a - high
    mid = rest.astype(BF16).astype(F32)
    return high, mid, rest - mid


def left_rows(a):
    high, mid, low = split3(a)
    return jnp.concatenate([high, high, high, mid, mid, low], axis=0)


def right_rows(a):
    high, mid, low = split3(a)
    return jnp.concatenate([high, mid, low, high, mid, high], axis=0)


def featured(x, q):
    row = rows_like(x.shape)
    square = jnp.sum(jnp.where(row < 3, x * x, 0.0), axis=0, keepdims=True)
    return jnp.where(
        row < 3, x, jnp.where(row == 3, square, jnp.where(row == 4, 1.0, jnp.where(row == 5, q, 0.0)))
    )


def partner_side(features, inverse):
    row = rows_like(features.shape)
    square = features[3:4, :]
    return jnp.where(
        row < 3,
        (2.0 * inverse) * features,
        jnp.where(row == 3, -inverse, jnp.where(row == 4, 1.0 - inverse * square, 0.0)),
    )


def pick_rows(features):
    count = len(features)
    shape = (KDIM, count * TILE)
    row, lane = rows_like(shape), lanes_like(shape)
    out = jnp.zeros(shape, F32)
    for block, f in enumerate(features):
        part = (row == f) | (row == 24 + f) | (row == 40 + f)
        out = jnp.where(part & (lane // TILE == block), 1.0, out)
    return out


def kernel(
    pos, vel, inv_mass, charge, fast, slow, bonds, bond_k, halo, own_slot, partner_slot, count,
    disp_out, vel_out, fast_out, slow_out,
    x_ref, v_ref, f_ref, start_ref, send, recv, left, right, near, incid, onehot, mult, total, slots,
    send_sem, recv_sem,
):
    place = [lax.axis_index(a) for a in AXES]
    extent = [lax.axis_size(a) for a in AXES]
    exists = []
    target = []
    for face in range(FACES):
        axis, high = face // 2, face % 2
        exists.append(place[axis] < extent[axis] - 1 if high else place[axis] > 0)
        target.append({AXES[axis]: place[axis] + 1 if high else place[axis] - 1})

    recv[...] = jnp.zeros_like(recv)

    barrier = pltpu.get_barrier_semaphore()
    for face in range(FACES):

        @pl.when(exists[face])
        def _(face=face):
            pl.semaphore_signal(barrier, inc=1, device_id=target[face], device_id_type=MESH)

    wide = (8, ATOMS)
    row = rows_like(wide)
    centre = jnp.where(
        row == 0, place[0].astype(F32), jnp.where(row == 1, place[1].astype(F32), place[2].astype(F32))
    ) * SIDE + 0.5 * SIDE
    x_ref[...] = jnp.zeros(wide, F32)
    v_ref[...] = jnp.zeros(wide, F32)
    f_ref[...] = jnp.zeros(wide, F32)
    x_ref[0:3, :] = pos[...] - centre[0:3, :]
    mass = inv_mass[...]
    v_ref[0:3, :] = vel[...] + (0.5 * INNER * STEP) * mass * slow[...]
    f_ref[0:3, :] = fast[...]
    start_ref[...] = x_ref[...]

    chunk = 128

    def build(c, _):
        base = pl.multiple_of(c * chunk, chunk)
        atom = rows_like((chunk, ATOMS)) + base
        first = jnp.where(atom == bonds[0:1, :], 1.0, 0.0)
        second = jnp.where(atom == bonds[1:2, :], 1.0, 0.0)
        incid[pl.ds(base, chunk), :] = (first - second).astype(BF16)
        atom = rows_like((chunk, HALO)) + base
        for face in range(FACES):
            hit = jnp.where(atom == halo[face : face + 1, :], 1.0, 0.0)
            onehot[pl.ds(base, chunk), face * HALO : (face + 1) * HALO] = hit.astype(BF16)
        return 0

    lax.fori_loop(0, ATOMS // chunk, build, 0)

    right[:, ATOMS : ATOMS + 4 * TILE] = pick_rows((0, 1, 2, 5)).astype(BF16)

    slots[...] = jnp.full(slots.shape, -1, jnp.int32)
    slots[0:1, 0:SLOTS] = own_slot[...]
    slots[1:2, 0:SLOTS] = partner_slot[...]
    slot_lane = lanes_like((ATOMS, 2 * TILE))
    tile_of = rows_like((ATOMS, 2 * TILE)) // TILE
    own_hit = jnp.where((tile_of == slots[0:1, :]) & (slot_lane < count[0, 0]), 1.0, 0.0).astype(BF16)
    partner_hit = jnp.where(rows_like((32, 2 * TILE)) == slots[1:2, :], 1.0, 0.0).astype(BF16)
    mult[...] = lax.dot_general(partner_hit, own_hit, (((1,), (1,)), ((), ())), preferred_element_type=F32)

    arrivals = exists[0].astype(jnp.int32)
    for face in range(1, FACES):
        arrivals = arrivals + exists[face].astype(jnp.int32)
    pl.semaphore_wait(barrier, arrivals)

    face_row = rows_like((8, HALO))

    def copy_out(k, face):
        return pltpu.make_async_remote_copy(
            src_ref=send.at[k, face],
            dst_ref=recv.at[k, face ^ 1],
            send_sem=send_sem.at[k, face],
            recv_sem=recv_sem.at[k, face ^ 1],
            device_id=target[face],
            device_id_type=MESH,
        )

    def short_blocks(first, last, acc):
        def one_block(b, acc):
            base = pl.multiple_of(b * BLOCK, BLOCK)
            near[:, 0 : ATOMS + 3 * TILE] = jnp.dot(
                left[pl.ds(base, BLOCK), :], right[:, 0 : ATOMS + 3 * TILE], preferred_element_type=F32
            )

            def group(g, acc):
                at = pl.ds(pl.multiple_of(g * 8, 8), 8)
                xj = [near[at, ATOMS + c * TILE : ATOMS + (c + 1) * TILE] for c in range(3)]
                out = []
                for t in range(OWN_TILES):
                    n = jnp.maximum(near[at, t * TILE : (t + 1) * TILE], 0.0)
                    s, fx, fy, fz = acc[4 * t : 4 * t + 4]
                    out += [s + n, fx + n * xj[0], fy + n * xj[1], fz + n * xj[2]]
                return tuple(out)

            return lax.fori_loop(0, BLOCK // 8, group, acc, unroll=8)

        return lax.fori_loop(first, last, one_block, acc)

    def gathered(acc, x):
        parts = []
        for t in range(OWN_TILES):
            s, fx, fy, fz = [jnp.sum(a, axis=0, keepdims=True) for a in acc[4 * t : 4 * t + 4]]
            r = rows_like((8, TILE))
            moved = jnp.where(r == 0, fx, jnp.where(r == 1, fy, jnp.where(r == 2, fz, 0.0)))
            parts.append(x[:, t * TILE : (t + 1) * TILE] * s - moved)
        return jnp.concatenate(parts, axis=1)

    zero_acc = tuple(jnp.zeros((8, TILE), F32) for _ in range(4 * OWN_TILES))

    def inner(k, _):
        v = v_ref[...] + (0.5 * STEP) * mass * f_ref[...]
        x = x_ref[...] + STEP * v
        v_ref[...] = v
        x_ref[...] = x
        features = featured(x, charge[...])
        rows = left_rows(features)
        high, mid, low = rows[0:8], rows[24:32], rows[40:48]
        parts = jnp.concatenate([high, mid, low], axis=0).astype(BF16)

        picked = jnp.dot(parts, onehot[...], preferred_element_type=F32)
        picked = picked[0:8] + picked[8:16] + picked[16:24]
        for face in range(FACES):
            send[k, face] = picked[:, face * HALO : (face + 1) * HALO]
        for face in range(FACES):

            @pl.when(exists[face])
            def _(face=face):
                copy_out(k, face).start()

        left[0:ATOMS, :] = rows.T.astype(BF16)
        right[:, 0:ATOMS] = right_rows(partner_side(features, SHORT_INV)).astype(BF16)

        apart = jnp.dot(parts, incid[...], preferred_element_type=F32)
        apart = apart[0:8] + apart[8:16] + apart[16:24]
        pull = split3(bond_k[...] * apart)
        pull = jnp.concatenate(pull, axis=0).astype(BF16)
        drawn = lax.dot_general(pull, incid[...], (((1,), (1,)), ((), ())), preferred_element_type=F32)
        f_ref[...] = -(drawn[0:8] + drawn[8:16] + drawn[16:24])

        acc = short_blocks(0, ATOMS // BLOCK, zero_acc)

        for face in range(FACES):

            @pl.when(exists[face])
            def _(face=face):
                copy_out(k, face ^ 1).wait_recv()

        for face in range(FACES):
            axis = face // 2
            shift = SIDE if face % 2 else -SIDE
            got = recv[k, face]
            seen = jnp.where(exists[face], jnp.ones((8, HALO), F32), 0.0) > 0.0
            moved = jnp.where(seen, got + jnp.where(face_row == axis, shift, 0.0), 0.0)
            there = featured(moved, moved[5:6, :])
            there = jnp.where(seen | (face_row != 3), there, FAR)
            base = ATOMS + face * HALO
            left[base : base + HALO, :] = left_rows(there).T.astype(BF16)

        acc = short_blocks(ATOMS // BLOCK, VISIBLE // BLOCK, acc)
        force = f_ref[...] + SHORT_SCALE * gathered(acc, x)
        force = jnp.where(row < 3, force, 0.0)
        f_ref[...] = force
        v_ref[...] = v_ref[...] + (0.5 * STEP) * mass * force

        for face in range(FACES):

            @pl.when(exists[face])
            def _(face=face):
                copy_out(k, face).wait_send()

        return 0

    lax.fori_loop(0, INNER, inner, 0)

    x = x_ref[...]
    features = featured(x, charge[...])
    right[:, 0:ATOMS] = right_rows(partner_side(features, LONG_INV)).astype(BF16)
    total[...] = jnp.zeros_like(total)

    def long_block(b, _):
        base = pl.multiple_of(b * TILE, TILE)
        near[0:TILE, :] = jnp.dot(left[pl.ds(base, TILE), :], right[...], preferred_element_type=F32)

        def group(g, acc):
            at = pl.ds(pl.multiple_of(g * 8, 8), 8)
            xj = [near[at, ATOMS + c * TILE : ATOMS + (c + 1) * TILE] for c in range(4)]
            out = []
            for t in range(OWN_TILES):
                n = jnp.maximum(near[at, t * TILE : (t + 1) * TILE], 0.0) * xj[3]
                s, fx, fy, fz = acc[4 * t : 4 * t + 4]
                out += [s + n, fx + n * xj[0], fy + n * xj[1], fz + n * xj[2]]
            return tuple(out)

        acc = lax.fori_loop(0, TILE // 8, group, zero_acc, unroll=8)
        times = mult[pl.ds(b, 1), :]
        for t in range(OWN_TILES):
            m = times[:, t * TILE : (t + 1) * TILE]
            for c in range(4):
                total[4 * t + c] = total[4 * t + c] + m * acc[4 * t + c]
        return 0

    lax.fori_loop(0, VISIBLE // TILE, long_block, 0)
    acc = [total[i] for i in range(4 * OWN_TILES)]
    slow_now = LONG_SCALE * charge[...] * gathered(acc, x)
    slow_out[...] = slow_now[0:3, :]
    fast_out[...] = f_ref[0:3, :]
    disp_out[...] = (x - start_ref[...])[0:3, :]
    vel_out[...] = v_ref[0:3, :] + (0.5 * INNER * STEP) * mass * slow_now[0:3, :]


def on_device(pos, vel, inv_mass, charge, fast, slow, bonds, bond_k, halo, own_slot, partner_slot, count):
    vmem = pl.BlockSpec(memory_space=pltpu.VMEM)
    smem = pl.BlockSpec(memory_space=pltpu.SMEM)
    out = jax.ShapeDtypeStruct((3, ATOMS), F32)
    return pl.pallas_call(
        kernel,
        out_shape=(out, out, out, out),
        in_specs=[vmem] * 11 + [smem],
        out_specs=(vmem,) * 4,
        scratch_shapes=[
            pltpu.VMEM((8, ATOMS), F32),
            pltpu.VMEM((8, ATOMS), F32),
            pltpu.VMEM((8, ATOMS), F32),
            pltpu.VMEM((8, ATOMS), F32),
            pltpu.VMEM((INNER, FACES, 8, HALO), F32),
            pltpu.VMEM((INNER, FACES, 8, HALO), F32),
            pltpu.VMEM((VISIBLE, KDIM), BF16),
            pltpu.VMEM((KDIM, ATOMS + 4 * TILE), BF16),
            pltpu.VMEM((BLOCK, ATOMS + 4 * TILE), F32),
            pltpu.VMEM((ATOMS, ATOMS), BF16),
            pltpu.VMEM((ATOMS, FACES * HALO), BF16),
            pltpu.VMEM((32, ATOMS), F32),
            pltpu.VMEM((4 * OWN_TILES, 8, TILE), F32),
            pltpu.VMEM((8, 2 * TILE), jnp.int32),
            pltpu.SemaphoreType.DMA((INNER, FACES)),
            pltpu.SemaphoreType.DMA((INNER, FACES)),
        ],
        compiler_params=pltpu.CompilerParams(collective_id=0, has_side_effects=True),
        name="outer_step",
    )(
        pos, vel, inv_mass[None, :], charge[None, :], fast, slow, bonds, bond_k[None, :], halo,
        own_slot[None, :], partner_slot[None, :], count[None, :],
    )


def solution(mesh):
    both = P(None, AXES)
    line = P(AXES)
    return jax.shard_map(
        on_device,
        mesh=mesh,
        in_specs=(both, both, line, line, both, both, both, line, both, line, line, line),
        out_specs=(both, both, both, both),
        check_vma=False,
    )
```

```python
import functools

import jax
import jax.numpy as jnp
from jax import lax
from jax.experimental import pallas as pl
from jax.experimental.pallas import tpu as pltpu
from jax.sharding import PartitionSpec as P

MESH = pl.DeviceIdType.MESH
F32 = jnp.float32
BF16 = jnp.bfloat16

INNER = 4
STEP = 0.1
SIDE = 4.0
SHORT_SCALE = 1.0
SHORT_INV = 1.0 / 0.64
LONG_SCALE = 0.5
LONG_INV = 1.0 / 1.44
FAR = 1e30

ATOMS = 1024
HALO = 256
FACES = 6
VISIBLE = ATOMS + FACES * HALO
BLOCK = 256
KDIM = 48
TILE = 128
OWN_TILES = ATOMS // TILE
SLOTS = 192
AXES = ("gx", "gy", "gz")


def rows_like(shape):
    return lax.broadcasted_iota(jnp.int32, shape, 0)


def lanes_like(shape):
    return lax.broadcasted_iota(jnp.int32, shape, 1)


def split3(a):
    high = a.astype(BF16).astype(F32)
    rest = a - high
    mid = rest.astype(BF16).astype(F32)
    return high, mid, rest - mid


def left_rows(a):
    high, mid, low = split3(a)
    return jnp.concatenate([high, high, high, mid, mid, low], axis=0)


def right_rows(a):
    high, mid, low = split3(a)
    return jnp.concatenate([high, mid, low, high, mid, high], axis=0)


def featured(x, q):
    row = rows_like(x.shape)
    square = jnp.sum(jnp.where(row < 3, x * x, 0.0), axis=0, keepdims=True)
    return jnp.where(
        row < 3, x, jnp.where(row == 3, square, jnp.where(row == 4, 1.0, jnp.where(row == 5, q, 0.0)))
    )


def partner_side(features, inverse):
    row = rows_like(features.shape)
    square = features[3:4, :]
    return jnp.where(
        row < 3,
        (2.0 * inverse) * features,
        jnp.where(row == 3, -inverse, jnp.where(row == 4, 1.0 - inverse * square, 0.0)),
    )


def pick_rows(features):
    count = len(features)
    shape = (KDIM, count * TILE)
    row, lane = rows_like(shape), lanes_like(shape)
    out = jnp.zeros(shape, F32)
    for block, f in enumerate(features):
        part = (row == f) | (row == 24 + f) | (row == 40 + f)
        out = jnp.where(part & (lane // TILE == block), 1.0, out)
    return out


def kernel(
    pos, vel, inv_mass, charge, fast, slow, bonds, bond_k, halo, own_slot, partner_slot, count,
    disp_out, vel_out, fast_out, slow_out,
    x_ref, v_ref, f_ref, start_ref, send, recv, left, right, spread, incid, mult, slots,
    send_sem, recv_sem,
):
    place = [lax.axis_index(a) for a in AXES]
    extent = [lax.axis_size(a) for a in AXES]
    exists = []
    target = []
    for face in range(FACES):
        axis, high = face // 2, face % 2
        exists.append(place[axis] < extent[axis] - 1 if high else place[axis] > 0)
        target.append({AXES[axis]: place[axis] + 1 if high else place[axis] - 1})

    recv[...] = jnp.zeros_like(recv)

    barrier = pltpu.get_barrier_semaphore()
    for face in range(FACES):

        @pl.when(exists[face])
        def _(face=face):
            pl.semaphore_signal(barrier, inc=1, device_id=target[face], device_id_type=MESH)

    wide = (8, ATOMS)
    row = rows_like(wide)
    centre = jnp.where(
        row == 0, place[0].astype(F32), jnp.where(row == 1, place[1].astype(F32), place[2].astype(F32))
    ) * SIDE + 0.5 * SIDE
    x_ref[...] = jnp.zeros(wide, F32)
    v_ref[...] = jnp.zeros(wide, F32)
    f_ref[...] = jnp.zeros(wide, F32)
    x_ref[0:3, :] = pos[...] - centre[0:3, :]
    mass = inv_mass[...]
    v_ref[0:3, :] = vel[...] + (0.5 * INNER * STEP) * mass * slow[...]
    f_ref[0:3, :] = fast[...]
    start_ref[...] = x_ref[...]

    stiff = jnp.where(bonds[0:1, :] == bonds[1:2, :], 0.0, bond_k[...])
    chunk = 128

    def build(c, _):
        base = pl.multiple_of(c * chunk, chunk)
        atom = rows_like((chunk, ATOMS)) + base
        sign = jnp.where(atom == bonds[0:1, :], 1.0, jnp.where(atom == bonds[1:2, :], -1.0, 0.0))
        incid[pl.ds(base, chunk), :] = sign.astype(BF16)
        return 0

    lax.fori_loop(0, ATOMS // chunk, build, 0)

    right[:, ATOMS : ATOMS + 4 * TILE] = pick_rows((0, 1, 2, 5)).astype(BF16)

    slots[...] = jnp.full(slots.shape, -1, jnp.int32)
    slots[0:1, 0:SLOTS] = own_slot[...]
    slots[1:2, 0:SLOTS] = partner_slot[...]
    slot_lane = lanes_like((ATOMS, 2 * TILE))
    tile_of = rows_like((ATOMS, 2 * TILE)) // TILE
    own_hit = jnp.where((tile_of == slots[0:1, :]) & (slot_lane < count[0, 0]), 1.0, 0.0).astype(BF16)
    partner_hit = jnp.where(rows_like((32, 2 * TILE)) == slots[1:2, :], 1.0, 0.0).astype(BF16)
    mult[...] = lax.dot_general(partner_hit, own_hit, (((1,), (1,)), ((), ())), preferred_element_type=F32)

    face_row = rows_like((8, HALO))

    def copy_out(k, face):
        return pltpu.make_async_remote_copy(
            src_ref=send.at[k, face],
            dst_ref=recv.at[k, face ^ 1],
            send_sem=send_sem.at[k, face],
            recv_sem=recv_sem.at[k, face ^ 1],
            device_id=target[face],
            device_id_type=MESH,
        )

    half = 2 * TILE

    def spread_rows(at, features):
        for f in features:
            cols = slice(f * TILE, (f + 1) * TILE)
            from_cols = slice(ATOMS + f * TILE, ATOMS + (f + 1) * TILE)
            spread[at, cols] = jnp.dot(left[at, :], right[:, from_cols], preferred_element_type=F32)

    def short_sum(base, count, acc):
        acc = list(acc)
        partners = left[pl.ds(base, count), :]
        for h in range(ATOMS // half):
            near = jnp.dot(partners, right[:, h * half : (h + 1) * half], preferred_element_type=F32)
            for g in range(count // 8):
                xj = [spread[pl.ds(base + 8 * g, 8), c * TILE : (c + 1) * TILE] for c in range(3)]
                for t in (2 * h, 2 * h + 1):
                    col = (t - 2 * h) * TILE
                    n = jnp.maximum(near[8 * g : 8 * g + 8, col : col + TILE], 0.0)
                    acc[4 * t] = acc[4 * t] + n
                    for c in range(3):
                        acc[4 * t + 1 + c] = acc[4 * t + 1 + c] + n * xj[c]
        return tuple(acc)

    def chosen(source, index):
        low = jnp.broadcast_to(index & (TILE - 1), (8, TILE))
        tile = jnp.broadcast_to(index >> 7, (8, TILE))
        out = jnp.zeros((8, TILE), F32)
        for t in range(OWN_TILES):
            cols = source[:, t * TILE : (t + 1) * TILE]
            out = jnp.where(tile == t, jnp.take_along_axis(cols, low, axis=1, mode="promise_in_bounds"), out)
        return out

    def advance():
        v = v_ref[...] + (0.5 * STEP) * mass * f_ref[...]
        x = x_ref[...] + STEP * v
        v_ref[...] = v
        x_ref[...] = x
        return jnp.where(row == 3, charge[...], x)

    def export(k, source):
        for face in range(FACES):
            for part in range(HALO // TILE):
                cols = slice(part * TILE, (part + 1) * TILE)
                send[k, face, :, cols] = chosen(source, halo[face : face + 1, cols])

    def gathered(acc, x):
        parts = []
        for t in range(OWN_TILES):
            s, fx, fy, fz = [jnp.sum(a, axis=0, keepdims=True) for a in acc[4 * t : 4 * t + 4]]
            r = rows_like((8, TILE))
            moved = jnp.where(r == 0, fx, jnp.where(r == 1, fy, jnp.where(r == 2, fz, 0.0)))
            parts.append(x[:, t * TILE : (t + 1) * TILE] * s - moved)
        return jnp.concatenate(parts, axis=1)

    zero_acc = tuple(jnp.zeros((8, TILE), F32) for _ in range(4 * OWN_TILES))

    odd_x, odd_z = lax.rem(place[0], 2), lax.rem(place[2], 2)
    far_x = (place[0] > 0) & (place[0] < extent[0] - 1)
    far_z = (place[2] > 0) & (place[2] < extent[2] - 1)
    arrivals_in_order = (
        (1, 2, exists[2], False),
        (1, 3, exists[3], False),
        (0, 1 - odd_x, None, True),
        (2, 5 - odd_z, None, True),
        (0, odd_x, far_x, False),
        (2, 4 + odd_z, far_z, False),
    )

    def absorb(k, axis, face, there, always):
        def landed():
            pltpu.make_async_remote_copy(
                src_ref=send.at[k, face],
                dst_ref=recv.at[k, face],
                send_sem=send_sem.at[k, face],
                recv_sem=recv_sem.at[k, face],
                device_id=target[2 * axis],
                device_id_type=MESH,
            ).wait_recv()

        if always:
            landed()
        else:
            pl.when(there)(landed)
        got = recv[k, face]
        shift = jnp.asarray(2 * lax.rem(face, 2) - 1, F32) * SIDE
        moved = got + jnp.where(face_row == axis, shift, 0.0)
        if always:
            block = featured(moved, got[3:4, :])
        else:
            seen = jnp.where(there, jnp.ones((8, HALO), F32), 0.0) > 0.0
            moved = jnp.where(seen, moved, 0.0)
            block = featured(moved, moved[3:4, :])
            block = jnp.where(seen | (face_row != 3), block, FAR)
        base = pl.multiple_of(ATOMS + face * HALO, HALO)
        left[pl.ds(base, HALO), :] = left_rows(block).T.astype(BF16)
        spread_rows(pl.ds(base, HALO), (0, 1, 2))

    export(0, advance())

    arrivals = exists[0].astype(jnp.int32)
    for face in range(1, FACES):
        arrivals = arrivals + exists[face].astype(jnp.int32)
    pl.semaphore_wait(barrier, arrivals)

    def inner(k, _):
        for face in range(FACES):

            @pl.when(exists[face])
            def _(face=face):
                copy_out(k, face).start()

        x = x_ref[...]
        features = featured(x, charge[...])
        rows = left_rows(features)
        left[0:ATOMS, :] = rows.T.astype(BF16)
        right[:, 0:ATOMS] = right_rows(partner_side(features, SHORT_INV)).astype(BF16)
        spread_rows(slice(0, ATOMS), (0, 1, 2))

        parts = jnp.concatenate([rows[0:8], rows[24:32], rows[40:48]], axis=0).astype(BF16)
        apart = jnp.dot(parts, incid[...], preferred_element_type=F32)
        apart = apart[0:8] + apart[8:16] + apart[16:24]
        pull = split3(stiff * apart)
        pull = jnp.concatenate(pull, axis=0).astype(BF16)
        drawn = lax.dot_general(pull, incid[...], (((1,), (1,)), ((), ())), preferred_element_type=F32)
        f_ref[...] = -(drawn[0:8] + drawn[8:16] + drawn[16:24])

        acc = short_sum(0, ATOMS, zero_acc)

        for pair in range(FACES // 2):
            now = arrivals_in_order[2 * pair : 2 * pair + 2]
            for axis, face, there, always in now:
                absorb(k, axis, face, there, always)
            for axis, face, there, always in now:
                acc = short_sum(pl.multiple_of(ATOMS + face * HALO, HALO), HALO, acc)

        force = f_ref[...] + SHORT_SCALE * gathered(acc, x)
        force = jnp.where(row < 3, force, 0.0)
        f_ref[...] = force
        v_ref[...] = v_ref[...] + (0.5 * STEP) * mass * force

        for face in range(FACES):

            @pl.when(exists[face])
            def _(face=face):
                copy_out(k, face).wait_send()

        @pl.when(k < INNER - 1)
        def _():
            export(k + 1, advance())

        return 0

    lax.fori_loop(0, INNER, inner, 0)

    x = x_ref[...]
    features = featured(x, charge[...])
    right[:, 0:ATOMS] = right_rows(partner_side(features, LONG_INV)).astype(BF16)
    spread_rows(slice(0, VISIBLE), (3,))
    acc = []
    for h in range(ATOMS // half):
        total = [jnp.zeros((8, TILE), F32) for _ in range(8)]
        for u in range(VISIBLE // TILE):
            partners = left[u * TILE : (u + 1) * TILE, :]
            near = jnp.dot(partners, right[:, h * half : (h + 1) * half], preferred_element_type=F32)
            part = [jnp.zeros((8, TILE), F32) for _ in range(8)]
            for g in range(TILE // 8):
                at = slice(u * TILE + 8 * g, u * TILE + 8 * g + 8)
                xj = [spread[at, c * TILE : (c + 1) * TILE] for c in range(4)]
                for t in range(2):
                    n = jnp.maximum(near[8 * g : 8 * g + 8, t * TILE : (t + 1) * TILE], 0.0) * xj[3]
                    part[4 * t] = part[4 * t] + n
                    for c in range(3):
                        part[4 * t + 1 + c] = part[4 * t + 1 + c] + n * xj[c]
            for t in range(2):
                m = mult[u : u + 1, h * half + t * TILE : h * half + (t + 1) * TILE]
                for c in range(4):
                    total[4 * t + c] = total[4 * t + c] + m * part[4 * t + c]
        acc += total
    slow_now = LONG_SCALE * charge[...] * gathered(acc, x)
    slow_out[...] = slow_now[0:3, :]
    fast_out[...] = f_ref[0:3, :]
    disp_out[...] = (x - start_ref[...])[0:3, :]
    vel_out[...] = v_ref[0:3, :] + (0.5 * INNER * STEP) * mass * slow_now[0:3, :]


def on_device(pos, vel, inv_mass, charge, fast, slow, bonds, bond_k, halo, own_slot, partner_slot, count):
    vmem = pl.BlockSpec(memory_space=pltpu.VMEM)
    smem = pl.BlockSpec(memory_space=pltpu.SMEM)
    out = jax.ShapeDtypeStruct((3, ATOMS), F32)
    return pl.pallas_call(
        kernel,
        out_shape=(out, out, out, out),
        in_specs=[vmem] * 11 + [smem],
        out_specs=(vmem,) * 4,
        scratch_shapes=[
            pltpu.VMEM((8, ATOMS), F32),
            pltpu.VMEM((8, ATOMS), F32),
            pltpu.VMEM((8, ATOMS), F32),
            pltpu.VMEM((8, ATOMS), F32),
            pltpu.VMEM((INNER, FACES, 8, HALO), F32),
            pltpu.VMEM((INNER, FACES, 8, HALO), F32),
            pltpu.VMEM((VISIBLE, KDIM), BF16),
            pltpu.VMEM((KDIM, ATOMS + 4 * TILE), BF16),
            pltpu.VMEM((VISIBLE, 4 * TILE), F32),
            pltpu.VMEM((ATOMS, ATOMS), BF16),
            pltpu.VMEM((32, ATOMS), F32),
            pltpu.VMEM((8, 2 * TILE), jnp.int32),
            pltpu.SemaphoreType.DMA((INNER, FACES)),
            pltpu.SemaphoreType.DMA((INNER, FACES)),
        ],
        compiler_params=pltpu.CompilerParams(collective_id=0, has_side_effects=True),
        name="outer_step",
    )(
        pos, vel, inv_mass[None, :], charge[None, :], fast, slow, bonds, bond_k[None, :], halo,
        own_slot[None, :], partner_slot[None, :], count[None, :],
    )


def solution(mesh):
    both = P(None, AXES)
    line = P(AXES)
    return jax.shard_map(
        on_device,
        mesh=mesh,
        in_specs=(both, both, line, line, both, both, both, line, both, line, line, line),
        out_specs=(both, both, both, both),
        check_vma=False,
    )
```

```python
import functools

import jax
import jax.numpy as jnp
from jax import lax
from jax.experimental import pallas as pl
from jax.experimental.pallas import tpu as pltpu
from jax.sharding import PartitionSpec as P

MESH = pl.DeviceIdType.MESH
F32 = jnp.float32
BF16 = jnp.bfloat16

INNER = 4
STEP = 0.1
SIDE = 4.0
SHORT_SCALE = 1.0
SHORT_INV = 1.0 / 0.64
LONG_SCALE = 0.5
LONG_INV = 1.0 / 1.44
FAR = 1e30

ATOMS = 1024
HALO = 256
FACES = 6
VISIBLE = ATOMS + FACES * HALO
BLOCK = 256
KDIM = 48
TILE = 128
OWN_TILES = ATOMS // TILE
SLOTS = 192
AXES = ("gx", "gy", "gz")
GROUPS = (ATOMS, HALO, 3 * HALO, 2 * HALO)


def rows_like(shape):
    return lax.broadcasted_iota(jnp.int32, shape, 0)


def lanes_like(shape):
    return lax.broadcasted_iota(jnp.int32, shape, 1)


def split3(a):
    high = a.astype(BF16).astype(F32)
    rest = a - high
    mid = rest.astype(BF16).astype(F32)
    return high, mid, rest - mid


def left_rows(a):
    high, mid, low = split3(a)
    return jnp.concatenate([high, high, high, mid, mid, low], axis=0)


def right_rows(a):
    high, mid, low = split3(a)
    return jnp.concatenate([high, mid, low, high, mid, high], axis=0)


def featured(x, q):
    row = rows_like(x.shape)
    square = jnp.sum(jnp.where(row < 3, x * x, 0.0), axis=0, keepdims=True)
    return jnp.where(
        row < 3, x, jnp.where(row == 3, square, jnp.where(row == 4, 1.0, jnp.where(row == 5, q, 0.0)))
    )


def partner_side(features, inverse):
    row = rows_like(features.shape)
    square = features[3:4, :]
    return jnp.where(
        row < 3,
        (2.0 * inverse) * features,
        jnp.where(row == 3, -inverse, jnp.where(row == 4, 1.0 - inverse * square, 0.0)),
    )


def pick_rows(features):
    count = len(features)
    shape = (KDIM, count * TILE)
    row, lane = rows_like(shape), lanes_like(shape)
    out = jnp.zeros(shape, F32)
    for block, f in enumerate(features):
        part = (row == f) | (row == 24 + f) | (row == 40 + f)
        out = jnp.where(part & (lane // TILE == block), 1.0, out)
    return out


def kernel(*refs):
    sources, count, packed_out, landing = refs[:11], refs[11], refs[12], refs[13]
    x_ref, v_ref, f_ref, start_ref, send, recv, lefts, spreads, right, incid, mult, slots = refs[14:26]
    send_sem, recv_sem, load_sem = refs[26:]
    pos, vel, inv_mass, charge, fast, slow, bonds, bond_k, halo, own_slot, partner_slot = landing
    loads = [pltpu.make_async_copy(a, b, load_sem.at[i]) for i, (a, b) in enumerate(zip(sources, landing))]
    for load in loads:
        load.start()

    place = [lax.axis_index(a) for a in AXES]
    extent = [lax.axis_size(a) for a in AXES]
    exists = []
    target = []
    for face in range(FACES):
        axis, high = face // 2, face % 2
        exists.append(place[axis] < extent[axis] - 1 if high else place[axis] > 0)
        target.append({AXES[axis]: place[axis] + 1 if high else place[axis] - 1})

    recv[...] = jnp.zeros_like(recv)

    barrier = pltpu.get_barrier_semaphore()
    for face in range(FACES):

        @pl.when(exists[face])
        def _(face=face):
            pl.semaphore_signal(barrier, inc=1, device_id=target[face], device_id_type=MESH)

    for load in loads:
        load.wait()

    wide = (8, ATOMS)
    row = rows_like(wide)
    centre = jnp.where(
        row == 0, place[0].astype(F32), jnp.where(row == 1, place[1].astype(F32), place[2].astype(F32))
    ) * SIDE + 0.5 * SIDE
    x_ref[...] = jnp.zeros(wide, F32)
    v_ref[...] = jnp.zeros(wide, F32)
    f_ref[...] = jnp.zeros(wide, F32)
    x_ref[0:3, :] = pos[...] - centre[0:3, :]
    mass = inv_mass[...]
    v_ref[0:3, :] = vel[...] + (0.5 * INNER * STEP) * mass * slow[...]
    f_ref[0:3, :] = fast[...]
    start_ref[...] = x_ref[...]

    stiff = jnp.where(bonds[0:1, :] == bonds[1:2, :], 0.0, bond_k[...])
    chunk = 128

    def build(c, _):
        base = pl.multiple_of(c * chunk, chunk)
        atom = rows_like((chunk, ATOMS)) + base
        sign = jnp.where(atom == bonds[0:1, :], 1.0, jnp.where(atom == bonds[1:2, :], -1.0, 0.0))
        incid[pl.ds(base, chunk), :] = sign.astype(BF16)
        return 0

    lax.fori_loop(0, ATOMS // chunk, build, 0)

    right[:, ATOMS : ATOMS + 4 * TILE] = pick_rows((0, 1, 2, 5)).astype(BF16)

    slots[...] = jnp.full(slots.shape, -1, jnp.int32)
    slots[0:1, 0:SLOTS] = own_slot[...]
    slots[1:2, 0:SLOTS] = partner_slot[...]
    slot_lane = lanes_like((ATOMS, 2 * TILE))
    tile_of = rows_like((ATOMS, 2 * TILE)) // TILE
    own_hit = jnp.where((tile_of == slots[0:1, :]) & (slot_lane < count[0, 0]), 1.0, 0.0).astype(BF16)
    partner_hit = jnp.where(rows_like((32, 2 * TILE)) == slots[1:2, :], 1.0, 0.0).astype(BF16)
    mult[...] = lax.dot_general(partner_hit, own_hit, (((1,), (1,)), ((), ())), preferred_element_type=F32)

    face_row = rows_like((8, HALO))

    def copy_out(k, face):
        return pltpu.make_async_remote_copy(
            src_ref=send.at[k, face],
            dst_ref=recv.at[k, face ^ 1],
            send_sem=send_sem.at[k, face],
            recv_sem=recv_sem.at[k, face ^ 1],
            device_id=target[face],
            device_id_type=MESH,
        )

    half = 2 * TILE

    def spread_rows(group, at, features):
        for f in features:
            cols = slice(f * TILE, (f + 1) * TILE)
            from_cols = slice(ATOMS + f * TILE, ATOMS + (f + 1) * TILE)
            spreads[group][at, cols] = jnp.dot(
                lefts[group][at, :], right[:, from_cols], preferred_element_type=F32
            )

    def short_sum(group, base, acc, beside=()):
        acc = list(acc)
        beside = list(beside)
        partners = lefts[group][base : base + BLOCK, :]
        for h in range(ATOMS // half):
            near = jnp.dot(partners, right[:, h * half : (h + 1) * half], preferred_element_type=F32)
            if beside:
                beside.pop(0)()
            for g in range(BLOCK // 8):
                at = slice(base + 8 * g, base + 8 * g + 8)
                xj = [spreads[group][at, c * TILE : (c + 1) * TILE] for c in range(3)]
                for t in (2 * h, 2 * h + 1):
                    col = (t - 2 * h) * TILE
                    n = jnp.maximum(near[8 * g : 8 * g + 8, col : col + TILE], 0.0)
                    acc[4 * t] = acc[4 * t] + n
                    for c in range(3):
                        acc[4 * t + 1 + c] = acc[4 * t + 1 + c] + n * xj[c]
        assert not beside
        return tuple(acc)

    def chosen(source, index):
        low = jnp.broadcast_to(index & (TILE - 1), (8, TILE))
        tile = jnp.broadcast_to(index >> 7, (8, TILE))
        out = jnp.zeros((8, TILE), F32)
        for t in range(OWN_TILES):
            cols = source[:, t * TILE : (t + 1) * TILE]
            out = jnp.where(tile == t, jnp.take_along_axis(cols, low, axis=1, mode="promise_in_bounds"), out)
        return out

    def advance():
        v = v_ref[...] + (0.5 * STEP) * mass * f_ref[...]
        x = x_ref[...] + STEP * v
        v_ref[...] = v
        x_ref[...] = x
        return jnp.where(row == 3, charge[...], x)

    def export(k, source):
        for face in range(FACES):
            for part in range(HALO // TILE):
                cols = slice(part * TILE, (part + 1) * TILE)
                send[k, face, :, cols] = chosen(source, halo[face : face + 1, cols])

    def gathered(acc, x):
        parts = []
        for t in range(OWN_TILES):
            s, fx, fy, fz = [jnp.sum(a, axis=0, keepdims=True) for a in acc[4 * t : 4 * t + 4]]
            r = rows_like((8, TILE))
            moved = jnp.where(r == 0, fx, jnp.where(r == 1, fy, jnp.where(r == 2, fz, 0.0)))
            parts.append(x[:, t * TILE : (t + 1) * TILE] * s - moved)
        return jnp.concatenate(parts, axis=1)

    zero_acc = tuple(jnp.zeros((8, TILE), F32) for _ in range(4 * OWN_TILES))

    odd_x, odd_z = lax.rem(place[0], 2), lax.rem(place[2], 2)
    far_x = (place[0] > 0) & (place[0] < extent[0] - 1)
    far_z = (place[2] > 0) & (place[2] < extent[2] - 1)
    groups = (
        ((2, 5 - odd_z, None),),
        ((1, 2, exists[2]), (1, 3, exists[3]), (0, 1 - odd_x, None)),
        ((0, odd_x, far_x), (2, 4 + odd_z, far_z)),
    )

    def landed(k, axis, face, there):
        def wait():
            pltpu.make_async_remote_copy(
                src_ref=send.at[k, face],
                dst_ref=recv.at[k, face],
                send_sem=send_sem.at[k, face],
                recv_sem=recv_sem.at[k, face],
                device_id=target[2 * axis],
                device_id_type=MESH,
            ).wait_recv()

        if there is None:
            wait()
        else:
            pl.when(there)(wait)

    def absorb(k, group, i):
        axis, face, there = groups[group - 1][i]
        got = recv[k, face]
        shift = jnp.asarray(2 * lax.rem(face, 2) - 1, F32) * SIDE
        moved = got + jnp.where(face_row == axis, shift, 0.0)
        if there is None:
            block = featured(moved, got[3:4, :])
        else:
            seen = jnp.where(there, jnp.ones((8, HALO), F32), 0.0) > 0.0
            moved = jnp.where(seen, moved, 0.0)
            block = featured(moved, moved[3:4, :])
            block = jnp.where(seen | (face_row != 3), block, FAR)
        at = slice(i * HALO, (i + 1) * HALO)
        lefts[group][at, :] = left_rows(block).T.astype(BF16)
        spread_rows(group, at, (0, 1, 2))

    export(0, advance())

    arrivals = exists[0].astype(jnp.int32)
    for face in range(1, FACES):
        arrivals = arrivals + exists[face].astype(jnp.int32)
    pl.semaphore_wait(barrier, arrivals)

    def inner(k, _):
        for face in range(FACES):

            @pl.when(exists[face])
            def _(face=face):
                copy_out(k, face).start()

        x = x_ref[...]
        features = featured(x, charge[...])
        rows = left_rows(features)
        right[:, 0:ATOMS] = right_rows(partner_side(features, SHORT_INV)).astype(BF16)
        parts = jnp.concatenate([rows[0:8], rows[24:32], rows[40:48]], axis=0).astype(BF16)

        def own(i):
            at = slice(i * BLOCK, (i + 1) * BLOCK)
            lefts[0][at, :] = rows[:, at].T.astype(BF16)
            spread_rows(0, at, (0, 1, 2))

        pulls = []

        def pull(i):
            at = slice(i * BLOCK, (i + 1) * BLOCK)
            apart = jnp.dot(parts, incid[:, at], preferred_element_type=F32)
            apart = stiff[:, at] * (apart[0:8] + apart[8:16] + apart[16:24])
            pulls.append(jnp.concatenate(split3(apart), axis=0).astype(BF16))

        def draw(i):
            at = slice(i * BLOCK, (i + 1) * BLOCK)
            pulled = jnp.concatenate(pulls, axis=1)
            drawn = lax.dot_general(
                pulled, incid[at, :], (((1,), (1,)), ((), ())), preferred_element_type=F32
            )
            f_ref[:, at] = -(drawn[0:8] + drawn[8:16] + drawn[16:24])

        def do(work, *what):
            return functools.partial(work, *what)

        own(0)
        acc = short_sum(0, 0, zero_acc, (do(own, 1), do(pull, 0), do(pull, 1)))
        acc = short_sum(0, BLOCK, acc, (do(own, 2), do(pull, 2), do(pull, 3)))

        for item in groups[0]:
            landed(k, *item)
        acc = short_sum(0, 2 * BLOCK, acc, (do(own, 3), do(absorb, k, 1, 0), do(draw, 0), do(draw, 1)))
        acc = short_sum(0, 3 * BLOCK, acc, (do(draw, 2), do(draw, 3)))

        for item in groups[1]:
            landed(k, *item)
        acc = short_sum(1, 0, acc, (do(absorb, k, 2, 0), do(absorb, k, 2, 1), do(absorb, k, 2, 2)))

        for item in groups[2]:
            landed(k, *item)
        acc = short_sum(2, 0, acc, (do(absorb, k, 3, 0), do(absorb, k, 3, 1)))
        acc = short_sum(2, BLOCK, acc)
        acc = short_sum(2, 2 * BLOCK, acc)
        acc = short_sum(3, 0, acc)
        acc = short_sum(3, BLOCK, acc)

        force = f_ref[...] + SHORT_SCALE * gathered(acc, x)
        force = jnp.where(row < 3, force, 0.0)
        f_ref[...] = force
        v_ref[...] = v_ref[...] + (0.5 * STEP) * mass * force

        for face in range(FACES):

            @pl.when(exists[face])
            def _(face=face):
                copy_out(k, face).wait_send()

        @pl.when(k < INNER - 1)
        def _():
            export(k + 1, advance())

        return 0

    lax.fori_loop(0, INNER, inner, 0)

    x = x_ref[...]
    features = featured(x, charge[...])
    right[:, 0:ATOMS] = right_rows(partner_side(features, LONG_INV)).astype(BF16)
    tiles = [(0, i, i) for i in range(OWN_TILES)]
    for group in (1, 2, 3):
        for i, (axis, face, there) in enumerate(groups[group - 1]):
            tiles += [(group, 2 * i + part, OWN_TILES + 2 * face + part) for part in range(2)]

    def spread_charge(at):
        if at < len(tiles):
            group, u, _ = tiles[at]
            spread_rows(group, slice(u * TILE, (u + 1) * TILE), (3,))

    spread_charge(0)
    acc = []
    for h in range(ATOMS // half):
        total = [jnp.zeros((8, TILE), F32) for _ in range(8)]
        for at_tile, (group, u, number) in enumerate(tiles):
            partners = lefts[group][u * TILE : (u + 1) * TILE, :]
            near = jnp.dot(partners, right[:, h * half : (h + 1) * half], preferred_element_type=F32)
            if h == 0:
                spread_charge(at_tile + 1)
            part = [jnp.zeros((8, TILE), F32) for _ in range(8)]
            for g in range(TILE // 8):
                at = slice(u * TILE + 8 * g, u * TILE + 8 * g + 8)
                xj = [spreads[group][at, c * TILE : (c + 1) * TILE] for c in range(4)]
                for t in range(2):
                    n = jnp.maximum(near[8 * g : 8 * g + 8, t * TILE : (t + 1) * TILE], 0.0) * xj[3]
                    part[4 * t] = part[4 * t] + n
                    for c in range(3):
                        part[4 * t + 1 + c] = part[4 * t + 1 + c] + n * xj[c]
            times = mult[pl.ds(number, 1), h * half : (h + 1) * half]
            for t in range(2):
                m = times[:, t * TILE : (t + 1) * TILE]
                for c in range(4):
                    total[4 * t + c] = total[4 * t + c] + m * part[4 * t + c]
        acc += total
    slow_now = LONG_SCALE * charge[...] * gathered(acc, x)
    packed_out[0:8, :] = x - start_ref[...]
    packed_out[8:16, :] = v_ref[...] + (0.5 * INNER * STEP) * mass * slow_now
    packed_out[16:24, :] = f_ref[...]
    packed_out[24:32, :] = slow_now


def finish(packed, disp_out, vel_out, fast_out, slow_out):
    disp_out[...] = packed[0:3, :]
    vel_out[...] = packed[8:11, :]
    fast_out[...] = packed[16:19, :]
    slow_out[...] = packed[24:27, :]


def on_device(pos, vel, inv_mass, charge, fast, slow, bonds, bond_k, halo, own_slot, partner_slot, count):
    vmem = pl.BlockSpec(memory_space=pltpu.VMEM)
    smem = pl.BlockSpec(memory_space=pltpu.SMEM)
    out = jax.ShapeDtypeStruct((3, ATOMS), F32)
    arrays = (
        pos, vel, inv_mass[None, :], charge[None, :], fast, slow, bonds, bond_k[None, :], halo,
        own_slot[None, :], partner_slot[None, :],
    )
    packed = pl.pallas_call(
        kernel,
        out_shape=jax.ShapeDtypeStruct((32, ATOMS), F32),
        in_specs=[pl.BlockSpec(memory_space=pltpu.HBM)] * 11 + [smem],
        out_specs=vmem,
        scratch_shapes=[
            [pltpu.VMEM(a.shape, a.dtype) for a in arrays],
            pltpu.VMEM((8, ATOMS), F32),
            pltpu.VMEM((8, ATOMS), F32),
            pltpu.VMEM((8, ATOMS), F32),
            pltpu.VMEM((8, ATOMS), F32),
            pltpu.VMEM((INNER, FACES, 8, HALO), F32),
            pltpu.VMEM((INNER, FACES, 8, HALO), F32),
            [pltpu.VMEM((count, KDIM), BF16) for count in GROUPS],
            [pltpu.VMEM((count, 4 * TILE), F32) for count in GROUPS],
            pltpu.VMEM((KDIM, ATOMS + 4 * TILE), BF16),
            pltpu.VMEM((ATOMS, ATOMS), BF16),
            pltpu.VMEM((32, ATOMS), F32),
            pltpu.VMEM((8, 2 * TILE), jnp.int32),
            pltpu.SemaphoreType.DMA((INNER, FACES)),
            pltpu.SemaphoreType.DMA((INNER, FACES)),
            pltpu.SemaphoreType.DMA((11,)),
        ],
        compiler_params=pltpu.CompilerParams(
            collective_id=0, has_side_effects=True
        ),
        name="outer_step",
    )(*arrays, count[None, :])
    return pl.pallas_call(
        finish,
        out_shape=(out, out, out, out),
        in_specs=[vmem],
        out_specs=(vmem,) * 4,

        name="finish",
    )(packed)


def solution(mesh):
    both = P(None, AXES)
    line = P(AXES)
    return jax.shard_map(
        on_device,
        mesh=mesh,
        in_specs=(both, both, line, line, both, both, both, line, both, line, line, line),
        out_specs=(both, both, both, both),
        check_vma=False,
    )
```

```python
import functools

import jax
import jax.numpy as jnp
from jax import lax
from jax.experimental import pallas as pl
from jax.experimental.pallas import tpu as pltpu
from jax.sharding import PartitionSpec as P

MESH = pl.DeviceIdType.MESH
F32 = jnp.float32
BF16 = jnp.bfloat16

INNER = 4
STEP = 0.1
SIDE = 4.0
SHORT_SCALE = 1.0
SHORT_INV = 1.0 / 0.64
LONG_SCALE = 0.5
LONG_INV = 1.0 / 1.44
FAR = 1e30

ATOMS = 1024
HALO = 256
FACES = 6
VISIBLE = ATOMS + FACES * HALO
BLOCK = 256
KDIM = 48
TILE = 128
OWN_TILES = ATOMS // TILE
SLOTS = 192
AXES = ("gx", "gy", "gz")
GROUPS = (ATOMS, HALO, 3 * HALO, 2 * HALO)


def rows_like(shape):
    return lax.broadcasted_iota(jnp.int32, shape, 0)


def lanes_like(shape):
    return lax.broadcasted_iota(jnp.int32, shape, 1)


def split3(a):
    high = a.astype(BF16).astype(F32)
    rest = a - high
    mid = rest.astype(BF16).astype(F32)
    return high, mid, rest - mid


def left_rows(a):
    high, mid, low = split3(a)
    return jnp.concatenate([high, high, high, mid, mid, low], axis=0)


def right_rows(a):
    high, mid, low = split3(a)
    return jnp.concatenate([high, mid, low, high, mid, high], axis=0)


def featured(x, q):
    row = rows_like(x.shape)
    square = jnp.sum(jnp.where(row < 3, x * x, 0.0), axis=0, keepdims=True)
    return jnp.where(
        row < 3, x, jnp.where(row == 3, square, jnp.where(row == 4, 1.0, jnp.where(row == 5, q, 0.0)))
    )


def partner_side(features, inverse):
    row = rows_like(features.shape)
    square = features[3:4, :]
    return jnp.where(
        row < 3,
        (2.0 * inverse) * features,
        jnp.where(row == 3, -inverse, jnp.where(row == 4, 1.0 - inverse * square, 0.0)),
    )


def pick_rows(features):
    count = len(features)
    shape = (KDIM, count * TILE)
    row, lane = rows_like(shape), lanes_like(shape)
    out = jnp.zeros(shape, F32)
    for block, f in enumerate(features):
        part = (row == f) | (row == 24 + f) | (row == 40 + f)
        out = jnp.where(part & (lane // TILE == block), 1.0, out)
    return out


def kernel(*refs):
    sources, count, packed_out, landing = refs[:11], refs[11], refs[12], refs[13]
    x_ref, v_ref, f_ref, start_ref, send, recv, lefts, spreads, right, incid, mult, slots = refs[14:26]
    send_sem, recv_sem, load_sem = refs[26:]
    pos, vel, inv_mass, charge, fast, slow, bonds, bond_k, halo, own_slot, partner_slot = landing
    loads = [pltpu.make_async_copy(a, b, load_sem.at[i]) for i, (a, b) in enumerate(zip(sources, landing))]
    for load in loads:
        load.start()

    place = [lax.axis_index(a) for a in AXES]
    extent = [lax.axis_size(a) for a in AXES]
    exists = []
    target = []
    for face in range(FACES):
        axis, high = face // 2, face % 2
        exists.append(place[axis] < extent[axis] - 1 if high else place[axis] > 0)
        target.append({AXES[axis]: place[axis] + 1 if high else place[axis] - 1})

    recv[...] = jnp.zeros_like(recv)

    barrier = pltpu.get_barrier_semaphore()
    for face in range(FACES):

        @pl.when(exists[face])
        def _(face=face):
            pl.semaphore_signal(barrier, inc=1, device_id=target[face], device_id_type=MESH)

    for load in loads:
        load.wait()

    wide = (8, ATOMS)
    row = rows_like(wide)
    centre = jnp.where(
        row == 0, place[0].astype(F32), jnp.where(row == 1, place[1].astype(F32), place[2].astype(F32))
    ) * SIDE + 0.5 * SIDE
    x_ref[...] = jnp.zeros(wide, F32)
    v_ref[...] = jnp.zeros(wide, F32)
    f_ref[...] = jnp.zeros(wide, F32)
    x_ref[0:3, :] = pos[...] - centre[0:3, :]
    mass = inv_mass[...]
    v_ref[0:3, :] = vel[...] + (0.5 * INNER * STEP) * mass * slow[...]
    f_ref[0:3, :] = fast[...]
    start_ref[...] = x_ref[...]

    stiff = jnp.where(bonds[0:1, :] == bonds[1:2, :], 0.0, bond_k[...])
    face_row = rows_like((8, HALO))

    def copy_out(k, axis, face):
        side = lax.rem(face, 2)
        over = face + 1 - 2 * side
        return pltpu.make_async_remote_copy(
            src_ref=send.at[k, face],
            dst_ref=recv.at[k, over],
            send_sem=send_sem.at[k, face],
            recv_sem=recv_sem.at[k, over],
            device_id={AXES[axis]: place[axis] + 2 * side - 1},
            device_id_type=MESH,
        )

    def when(there, action):
        if there is None:
            action()
        else:
            pl.when(there)(action)

    half = 2 * TILE

    def spread_rows(group, at, features):
        for f in features:
            cols = slice(f * TILE, (f + 1) * TILE)
            from_cols = slice(ATOMS + f * TILE, ATOMS + (f + 1) * TILE)
            spreads[group][at, cols] = jnp.dot(
                lefts[group][at, :], right[:, from_cols], preferred_element_type=F32
            )

    def short_sum(group, base, acc, beside=()):
        acc = list(acc)
        beside = list(beside)
        partners = lefts[group][base : base + BLOCK, :]
        for h in range(ATOMS // half):
            near = jnp.dot(partners, right[:, h * half : (h + 1) * half], preferred_element_type=F32)
            if beside:
                beside.pop(0)()
            for g in range(BLOCK // 8):
                at = slice(base + 8 * g, base + 8 * g + 8)
                xj = [spreads[group][at, c * TILE : (c + 1) * TILE] for c in range(3)]
                for t in (2 * h, 2 * h + 1):
                    col = (t - 2 * h) * TILE
                    n = jnp.maximum(near[8 * g : 8 * g + 8, col : col + TILE], 0.0)
                    acc[4 * t] = acc[4 * t] + n
                    for c in range(3):
                        acc[4 * t + 1 + c] = acc[4 * t + 1 + c] + n * xj[c]
        assert not beside
        return tuple(acc)

    def chosen(source, index):
        low = jnp.broadcast_to(index & (TILE - 1), (8, TILE))
        tile = jnp.broadcast_to(index >> 7, (8, TILE))
        out = jnp.zeros((8, TILE), F32)
        for t in range(OWN_TILES):
            cols = source[:, t * TILE : (t + 1) * TILE]
            out = jnp.where(tile == t, jnp.take_along_axis(cols, low, axis=1, mode="promise_in_bounds"), out)
        return out

    def advance():
        v = v_ref[...] + (0.5 * STEP) * mass * f_ref[...]
        x = x_ref[...] + STEP * v
        v_ref[...] = v
        x_ref[...] = x
        return jnp.where(row == 3, charge[...], x)

    def export(k, source):
        for face in range(FACES):
            for part in range(HALO // TILE):
                cols = slice(part * TILE, (part + 1) * TILE)
                send[k, face, :, cols] = chosen(source, halo[face : face + 1, cols])[0:4, :]

    def gathered(acc, x):
        parts = []
        for t in range(OWN_TILES):
            s, fx, fy, fz = [jnp.sum(a, axis=0, keepdims=True) for a in acc[4 * t : 4 * t + 4]]
            r = rows_like((8, TILE))
            moved = jnp.where(r == 0, fx, jnp.where(r == 1, fy, jnp.where(r == 2, fz, 0.0)))
            parts.append(x[:, t * TILE : (t + 1) * TILE] * s - moved)
        return jnp.concatenate(parts, axis=1)

    zero_acc = tuple(jnp.zeros((8, TILE), F32) for _ in range(4 * OWN_TILES))

    odd_x, odd_z = lax.rem(place[0], 2), lax.rem(place[2], 2)
    far_x = (place[0] > 0) & (place[0] < extent[0] - 1)
    far_z = (place[2] > 0) & (place[2] < extent[2] - 1)
    groups = (
        ((2, 5 - odd_z, None),),
        ((1, 2, exists[2]), (1, 3, exists[3]), (0, 1 - odd_x, None)),
        ((0, odd_x, far_x), (2, 4 + odd_z, far_z)),
    )

    def landed(k, axis, face, there):
        def wait():
            pltpu.make_async_remote_copy(
                src_ref=send.at[k, face],
                dst_ref=recv.at[k, face],
                send_sem=send_sem.at[k, face],
                recv_sem=recv_sem.at[k, face],
                device_id=target[2 * axis],
                device_id_type=MESH,
            ).wait_recv()

        when(there, wait)

    def absorb(k, group, i):
        axis, face, there = groups[group - 1][i]
        got = recv[k, face]
        got = jnp.concatenate([got, jnp.zeros_like(got)], axis=0)
        shift = jnp.asarray(2 * lax.rem(face, 2) - 1, F32) * SIDE
        moved = got + jnp.where(face_row == axis, shift, 0.0)
        if there is None:
            block = featured(moved, got[3:4, :])
        else:
            seen = jnp.where(there, jnp.ones((8, HALO), F32), 0.0) > 0.0
            moved = jnp.where(seen, moved, 0.0)
            block = featured(moved, moved[3:4, :])
            block = jnp.where(seen | (face_row != 3), block, FAR)
        at = slice(i * HALO, (i + 1) * HALO)
        lefts[group][at, :] = left_rows(block).T.astype(BF16)
        spread_rows(group, at, (0, 1, 2))

    export(0, advance())

    arrivals = exists[0].astype(jnp.int32)
    for face in range(1, FACES):
        arrivals = arrivals + exists[face].astype(jnp.int32)
    pl.semaphore_wait(barrier, arrivals)

    def tables():
        chunk = 128

        def build(c, _):
            base = pl.multiple_of(c * chunk, chunk)
            atom = rows_like((chunk, ATOMS)) + base
            sign = jnp.where(atom == bonds[0:1, :], 1.0, jnp.where(atom == bonds[1:2, :], -1.0, 0.0))
            incid[pl.ds(base, chunk), :] = sign.astype(BF16)
            return 0

        lax.fori_loop(0, ATOMS // chunk, build, 0)

        right[:, ATOMS : ATOMS + 4 * TILE] = pick_rows((0, 1, 2, 5)).astype(BF16)

        slots[...] = jnp.full(slots.shape, -1, jnp.int32)
        slots[0:1, 0:SLOTS] = own_slot[...]
        slots[1:2, 0:SLOTS] = partner_slot[...]
        slot_lane = lanes_like((ATOMS, 2 * TILE))
        tile_of = rows_like((ATOMS, 2 * TILE)) // TILE
        own_hit = jnp.where((tile_of == slots[0:1, :]) & (slot_lane < count[0, 0]), 1.0, 0.0).astype(BF16)
        partner_hit = jnp.where(rows_like((32, 2 * TILE)) == slots[1:2, :], 1.0, 0.0).astype(BF16)
        mult[...] = lax.dot_general(partner_hit, own_hit, (((1,), (1,)), ((), ())), preferred_element_type=F32)

    def inner(k, _):
        for axis, face, there in groups[2] + groups[1] + groups[0]:
            when(there, lambda axis=axis, face=face: copy_out(k, axis, face).start())

        pl.when(k == 0)(tables)

        x = x_ref[...]
        features = featured(x, charge[...])
        rows = left_rows(features)
        right[:, 0:ATOMS] = right_rows(partner_side(features, SHORT_INV)).astype(BF16)
        parts = jnp.concatenate([rows[0:8], rows[24:32], rows[40:48]], axis=0).astype(BF16)

        def own(i):
            at = slice(i * BLOCK, (i + 1) * BLOCK)
            lefts[0][at, :] = rows[:, at].T.astype(BF16)
            spread_rows(0, at, (0, 1, 2))

        pulls = []

        def pull(i):
            at = slice(i * BLOCK, (i + 1) * BLOCK)
            apart = jnp.dot(parts, incid[:, at], preferred_element_type=F32)
            apart = stiff[:, at] * (apart[0:8] + apart[8:16] + apart[16:24])
            pulls.append(jnp.concatenate(split3(apart), axis=0).astype(BF16))

        def draw(i):
            at = slice(i * BLOCK, (i + 1) * BLOCK)
            pulled = jnp.concatenate(pulls, axis=1)
            drawn = lax.dot_general(
                pulled, incid[at, :], (((1,), (1,)), ((), ())), preferred_element_type=F32
            )
            f_ref[:, at] = -(drawn[0:8] + drawn[8:16] + drawn[16:24])

        def do(work, *what):
            return functools.partial(work, *what)

        own(0)
        acc = short_sum(0, 0, zero_acc, (do(own, 1), do(pull, 0), do(pull, 1)))
        acc = short_sum(0, BLOCK, acc, (do(own, 2), do(pull, 2), do(pull, 3)))

        for item in groups[0]:
            landed(k, *item)
        acc = short_sum(0, 2 * BLOCK, acc, (do(own, 3), do(absorb, k, 1, 0), do(draw, 0), do(draw, 1)))
        acc = short_sum(0, 3 * BLOCK, acc, (do(draw, 2), do(draw, 3)))

        for axis, face, there in groups[2] + groups[1] + groups[0]:
            when(there, lambda axis=axis, face=face: copy_out(k, axis, face).wait_send())
        for item in groups[1]:
            landed(k, *item)
        acc = short_sum(1, 0, acc, (do(absorb, k, 2, 0), do(absorb, k, 2, 1), do(absorb, k, 2, 2)))

        acc = short_sum(2, 0, acc)
        acc = short_sum(2, BLOCK, acc)

        for item in groups[2]:
            landed(k, *item)
        acc = short_sum(2, 2 * BLOCK, acc, (do(absorb, k, 3, 0), do(absorb, k, 3, 1)))
        acc = short_sum(3, 0, acc)
        acc = short_sum(3, BLOCK, acc)

        force = f_ref[...] + SHORT_SCALE * gathered(acc, x)
        force = jnp.where(row < 3, force, 0.0)
        f_ref[...] = force
        v_ref[...] = v_ref[...] + (0.5 * STEP) * mass * force

        @pl.when(k < INNER - 1)
        def _():
            export(k + 1, advance())

        return 0

    lax.fori_loop(0, INNER, inner, 0)

    x = x_ref[...]
    features = featured(x, charge[...])
    right[:, 0:ATOMS] = right_rows(partner_side(features, LONG_INV)).astype(BF16)
    tiles = [(0, i, i) for i in range(OWN_TILES)]
    for group in (1, 2, 3):
        for i, (axis, face, there) in enumerate(groups[group - 1]):
            tiles += [(group, 2 * i + part, OWN_TILES + 2 * face + part) for part in range(2)]

    def spread_charge(at):
        if at < len(tiles):
            group, u, _ = tiles[at]
            spread_rows(group, slice(u * TILE, (u + 1) * TILE), (3,))

    spread_charge(0)
    acc = []
    for h in range(ATOMS // half):
        total = [jnp.zeros((8, TILE), F32) for _ in range(8)]
        for at_tile, (group, u, number) in enumerate(tiles):
            partners = lefts[group][u * TILE : (u + 1) * TILE, :]
            near = jnp.dot(partners, right[:, h * half : (h + 1) * half], preferred_element_type=F32)
            if h == 0:
                spread_charge(at_tile + 1)
            part = [jnp.zeros((8, TILE), F32) for _ in range(8)]
            for g in range(TILE // 8):
                at = slice(u * TILE + 8 * g, u * TILE + 8 * g + 8)
                xj = [spreads[group][at, c * TILE : (c + 1) * TILE] for c in range(4)]
                for t in range(2):
                    n = jnp.maximum(near[8 * g : 8 * g + 8, t * TILE : (t + 1) * TILE], 0.0) * xj[3]
                    part[4 * t] = part[4 * t] + n
                    for c in range(3):
                        part[4 * t + 1 + c] = part[4 * t + 1 + c] + n * xj[c]
            times = mult[pl.ds(number, 1), h * half : (h + 1) * half]
            for t in range(2):
                m = times[:, t * TILE : (t + 1) * TILE]
                for c in range(4):
                    total[4 * t + c] = total[4 * t + c] + m * part[4 * t + c]
        acc += total
    slow_now = LONG_SCALE * charge[...] * gathered(acc, x)
    packed_out[0:8, :] = x - start_ref[...]
    packed_out[8:16, :] = v_ref[...] + (0.5 * INNER * STEP) * mass * slow_now
    packed_out[16:24, :] = f_ref[...]
    packed_out[24:32, :] = slow_now


def finish(packed, disp_out, vel_out, fast_out, slow_out):
    disp_out[...] = packed[0:3, :]
    vel_out[...] = packed[8:11, :]
    fast_out[...] = packed[16:19, :]
    slow_out[...] = packed[24:27, :]


def on_device(pos, vel, inv_mass, charge, fast, slow, bonds, bond_k, halo, own_slot, partner_slot, count):
    vmem = pl.BlockSpec(memory_space=pltpu.VMEM)
    smem = pl.BlockSpec(memory_space=pltpu.SMEM)
    out = jax.ShapeDtypeStruct((3, ATOMS), F32)
    arrays = (
        pos, vel, inv_mass[None, :], charge[None, :], fast, slow, bonds, bond_k[None, :], halo,
        own_slot[None, :], partner_slot[None, :],
    )
    packed = pl.pallas_call(
        kernel,
        out_shape=pltpu.VMEM((32, ATOMS), F32),
        in_specs=[pl.BlockSpec(memory_space=pltpu.HBM)] * 11 + [smem],
        out_specs=vmem,
        scratch_shapes=[
            [pltpu.VMEM(a.shape, a.dtype) for a in arrays],
            pltpu.VMEM((8, ATOMS), F32),
            pltpu.VMEM((8, ATOMS), F32),
            pltpu.VMEM((8, ATOMS), F32),
            pltpu.VMEM((8, ATOMS), F32),
            pltpu.VMEM((INNER, FACES, 4, HALO), F32),
            pltpu.VMEM((INNER, FACES, 4, HALO), F32),
            [pltpu.VMEM((count, KDIM), BF16) for count in GROUPS],
            [pltpu.VMEM((count, 4 * TILE), F32) for count in GROUPS],
            pltpu.VMEM((KDIM, ATOMS + 4 * TILE), BF16),
            pltpu.VMEM((ATOMS, ATOMS), BF16),
            pltpu.VMEM((32, ATOMS), F32),
            pltpu.VMEM((8, 2 * TILE), jnp.int32),
            pltpu.SemaphoreType.DMA((INNER, FACES)),
            pltpu.SemaphoreType.DMA((INNER, FACES)),
            pltpu.SemaphoreType.DMA((11,)),
        ],
        compiler_params=pltpu.CompilerParams(
            collective_id=0, has_side_effects=True
        ),
        name="outer_step",
    )(*arrays, count[None, :])
    return pl.pallas_call(
        finish,
        out_shape=(out, out, out, out),
        in_specs=[vmem],
        out_specs=(vmem,) * 4,

        compiler_params=pltpu.CompilerParams(vmem_limit_bytes=4 * 1024 * 1024),
        name="finish",
    )(packed)


def solution(mesh):
    both = P(None, AXES)
    line = P(AXES)
    return jax.shard_map(
        on_device,
        mesh=mesh,
        in_specs=(both, both, line, line, both, both, both, line, both, line, line, line),
        out_specs=(both, both, both, both),
        check_vma=False,
    )
```

```python
import functools

import jax
import jax.numpy as jnp
from jax import lax
from jax.experimental import pallas as pl
from jax.experimental.pallas import tpu as pltpu
from jax.sharding import PartitionSpec as P

MESH = pl.DeviceIdType.MESH
F32 = jnp.float32
BF16 = jnp.bfloat16

INNER = 4
STEP = 0.1
SIDE = 4.0
SHORT_SCALE = 1.0
SHORT_INV = 1.0 / 0.64
LONG_SCALE = 0.5
LONG_INV = 1.0 / 1.44
FAR = 1e30

ATOMS = 1024
HALO = 256
FACES = 6
VISIBLE = ATOMS + FACES * HALO
BLOCK = 256
KDIM = 48
TILE = 128
OWN_TILES = ATOMS // TILE
SLOTS = 192
AXES = ("gx", "gy", "gz")
GROUPS = (ATOMS, HALO, 3 * HALO, 2 * HALO)


def rows_like(shape):
    return lax.broadcasted_iota(jnp.int32, shape, 0)


def lanes_like(shape):
    return lax.broadcasted_iota(jnp.int32, shape, 1)


def split3(a):
    high = a.astype(BF16).astype(F32)
    rest = a - high
    mid = rest.astype(BF16).astype(F32)
    return high, mid, rest - mid


def left_rows(a):
    high, mid, low = split3(a)
    return jnp.concatenate([high, high, high, mid, mid, low], axis=0)


def right_rows(a):
    high, mid, low = split3(a)
    return jnp.concatenate([high, mid, low, high, mid, high], axis=0)


def featured(x, q):
    row = rows_like(x.shape)
    square = jnp.sum(jnp.where(row < 3, x * x, 0.0), axis=0, keepdims=True)
    return jnp.where(
        row < 3, x, jnp.where(row == 3, square, jnp.where(row == 4, 1.0, jnp.where(row == 5, q, 0.0)))
    )


def partner_side(features, inverse):
    row = rows_like(features.shape)
    square = features[3:4, :]
    return jnp.where(
        row < 3,
        (2.0 * inverse) * features,
        jnp.where(row == 3, -inverse, jnp.where(row == 4, 1.0 - inverse * square, 0.0)),
    )


def pick_rows(features):
    count = len(features)
    shape = (KDIM, count * TILE)
    row, lane = rows_like(shape), lanes_like(shape)
    out = jnp.zeros(shape, F32)
    for block, f in enumerate(features):
        part = (row == f) | (row == 24 + f) | (row == 40 + f)
        out = jnp.where(part & (lane // TILE == block), 1.0, out)
    return out


def kernel(*refs):
    sources, count, packed_out, landing = refs[:11], refs[11], refs[12], refs[13]
    x_ref, v_ref, f_ref, start_ref, send, recv, lefts, spreads, right, incid, mult, slots = refs[14:26]
    send_sem, recv_sem, load_sem = refs[26:]
    pos, vel, inv_mass, charge, fast, slow, bonds, bond_k, halo, own_slot, partner_slot = landing
    loads = [pltpu.make_async_copy(a, b, load_sem.at[i]) for i, (a, b) in enumerate(zip(sources, landing))]
    for load in loads:
        load.start()

    place = [lax.axis_index(a) for a in AXES]
    extent = [lax.axis_size(a) for a in AXES]
    exists = []
    target = []
    for face in range(FACES):
        axis, high = face // 2, face % 2
        exists.append(place[axis] < extent[axis] - 1 if high else place[axis] > 0)
        target.append({AXES[axis]: place[axis] + 1 if high else place[axis] - 1})

    recv[...] = jnp.zeros_like(recv)

    barrier = pltpu.get_barrier_semaphore()
    for face in range(FACES):

        @pl.when(exists[face])
        def _(face=face):
            pl.semaphore_signal(barrier, inc=1, device_id=target[face], device_id_type=MESH)

    for load in loads:
        load.wait()

    wide = (8, ATOMS)
    row = rows_like(wide)
    centre = jnp.where(
        row == 0, place[0].astype(F32), jnp.where(row == 1, place[1].astype(F32), place[2].astype(F32))
    ) * SIDE + 0.5 * SIDE
    x_ref[...] = jnp.zeros(wide, F32)
    v_ref[...] = jnp.zeros(wide, F32)
    f_ref[...] = jnp.zeros(wide, F32)
    x_ref[0:3, :] = pos[...] - centre[0:3, :]
    mass = inv_mass[...]
    v_ref[0:3, :] = vel[...] + (0.5 * INNER * STEP) * mass * slow[...]
    f_ref[0:3, :] = fast[...]
    start_ref[...] = x_ref[...]

    stiff = jnp.where(bonds[0:1, :] == bonds[1:2, :], 0.0, bond_k[...])
    face_row = rows_like((8, HALO))

    def copy_out(k, axis, face):
        side = lax.rem(face, 2)
        over = face + 1 - 2 * side
        return pltpu.make_async_remote_copy(
            src_ref=send.at[k, face],
            dst_ref=recv.at[k, over],
            send_sem=send_sem.at[k, face],
            recv_sem=recv_sem.at[k, over],
            device_id={AXES[axis]: place[axis] + 2 * side - 1},
            device_id_type=MESH,
        )

    def when(there, action):
        if there is None:
            action()
        else:
            pl.when(there)(action)

    half = 2 * TILE

    def spread_rows(group, at, features):
        for f in features:
            cols = slice(f * TILE, (f + 1) * TILE)
            from_cols = slice(ATOMS + f * TILE, ATOMS + (f + 1) * TILE)
            spreads[group][at, cols] = jnp.dot(
                lefts[group][at, :], right[:, from_cols], preferred_element_type=F32
            )

    def short_sum(group, base, acc, beside=()):
        acc = list(acc)
        beside = list(beside)
        partners = lefts[group][base : base + BLOCK, :]
        for h in range(ATOMS // half):
            near = jnp.dot(partners, right[:, h * half : (h + 1) * half], preferred_element_type=F32)
            if beside:
                beside.pop(0)()
            for g in range(BLOCK // 8):
                at = slice(base + 8 * g, base + 8 * g + 8)
                xj = [spreads[group][at, c * TILE : (c + 1) * TILE] for c in range(3)]
                for t in (2 * h, 2 * h + 1):
                    col = (t - 2 * h) * TILE
                    n = jnp.maximum(near[8 * g : 8 * g + 8, col : col + TILE], 0.0)
                    acc[4 * t] = acc[4 * t] + n
                    for c in range(3):
                        acc[4 * t + 1 + c] = acc[4 * t + 1 + c] + n * xj[c]
        assert not beside
        return tuple(acc)

    def chosen(packed, index):
        low = jnp.broadcast_to(index & (TILE - 1), (8, TILE))
        tile = jnp.broadcast_to(index >> 7, (8, TILE))
        out = jnp.zeros((8, TILE), F32)
        for t in range(OWN_TILES // 2):
            cols = packed[:, t * TILE : (t + 1) * TILE]
            found = jnp.take_along_axis(cols, low, axis=1, mode="promise_in_bounds")
            out = jnp.where((tile & 3) == t, found, out)
        return jnp.where(tile[0:4] < OWN_TILES // 2, out[0:4], out[4:8])

    def advance():
        v = v_ref[...] + (0.5 * STEP) * mass * f_ref[...]
        x = x_ref[...] + STEP * v
        v_ref[...] = v
        x_ref[...] = x
        return jnp.where(row == 3, charge[...], x)

    def export(k, source):
        packed = jnp.concatenate([source[0:4, : ATOMS // 2], source[0:4, ATOMS // 2 :]], axis=0)
        for face in range(FACES):
            for part in range(HALO // TILE):
                cols = slice(part * TILE, (part + 1) * TILE)
                send[k, face, :, cols] = chosen(packed, halo[face : face + 1, cols])

    def gathered(acc, x):
        parts = []
        for t in range(OWN_TILES):
            s, fx, fy, fz = [jnp.sum(a, axis=0, keepdims=True) for a in acc[4 * t : 4 * t + 4]]
            r = rows_like((8, TILE))
            moved = jnp.where(r == 0, fx, jnp.where(r == 1, fy, jnp.where(r == 2, fz, 0.0)))
            parts.append(x[:, t * TILE : (t + 1) * TILE] * s - moved)
        return jnp.concatenate(parts, axis=1)

    zero_acc = tuple(jnp.zeros((8, TILE), F32) for _ in range(4 * OWN_TILES))

    odd_x, odd_z = lax.rem(place[0], 2), lax.rem(place[2], 2)
    far_x = (place[0] > 0) & (place[0] < extent[0] - 1)
    far_z = (place[2] > 0) & (place[2] < extent[2] - 1)
    groups = (
        ((2, 5 - odd_z, None),),
        ((1, 2, exists[2]), (1, 3, exists[3]), (0, 1 - odd_x, None)),
        ((0, odd_x, far_x), (2, 4 + odd_z, far_z)),
    )

    def landed(k, axis, face, there):
        def wait():
            pltpu.make_async_remote_copy(
                src_ref=send.at[k, face],
                dst_ref=recv.at[k, face],
                send_sem=send_sem.at[k, face],
                recv_sem=recv_sem.at[k, face],
                device_id=target[2 * axis],
                device_id_type=MESH,
            ).wait_recv()

        when(there, wait)

    def absorb(k, group, i):
        axis, face, there = groups[group - 1][i]
        got = recv[k, face]
        got = jnp.concatenate([got, jnp.zeros_like(got)], axis=0)
        shift = jnp.asarray(2 * lax.rem(face, 2) - 1, F32) * SIDE
        moved = got + jnp.where(face_row == axis, shift, 0.0)
        if there is None:
            block = featured(moved, got[3:4, :])
        else:
            seen = jnp.where(there, jnp.ones((8, HALO), F32), 0.0) > 0.0
            moved = jnp.where(seen, moved, 0.0)
            block = featured(moved, moved[3:4, :])
            block = jnp.where(seen | (face_row != 3), block, FAR)
        at = slice(i * HALO, (i + 1) * HALO)
        lefts[group][at, :] = left_rows(block).T.astype(BF16)
        spread_rows(group, at, (0, 1, 2))

    export(0, advance())

    arrivals = exists[0].astype(jnp.int32)
    for face in range(1, FACES):
        arrivals = arrivals + exists[face].astype(jnp.int32)
    pl.semaphore_wait(barrier, arrivals)

    def tables():
        chunk = 128

        def build(c, _):
            base = pl.multiple_of(c * chunk, chunk)
            atom = rows_like((chunk, ATOMS)) + base
            sign = jnp.where(atom == bonds[0:1, :], 1.0, jnp.where(atom == bonds[1:2, :], -1.0, 0.0))
            incid[pl.ds(base, chunk), :] = sign.astype(BF16)
            return 0

        lax.fori_loop(0, ATOMS // chunk, build, 0)

        right[:, ATOMS : ATOMS + 4 * TILE] = pick_rows((0, 1, 2, 5)).astype(BF16)

        slots[...] = jnp.full(slots.shape, -1, jnp.int32)
        slots[0:1, 0:SLOTS] = own_slot[...]
        slots[1:2, 0:SLOTS] = partner_slot[...]
        slot_lane = lanes_like((ATOMS, 2 * TILE))
        tile_of = rows_like((ATOMS, 2 * TILE)) // TILE
        own_hit = jnp.where((tile_of == slots[0:1, :]) & (slot_lane < count[0, 0]), 1.0, 0.0).astype(BF16)
        partner_hit = jnp.where(rows_like((32, 2 * TILE)) == slots[1:2, :], 1.0, 0.0).astype(BF16)
        mult[...] = lax.dot_general(partner_hit, own_hit, (((1,), (1,)), ((), ())), preferred_element_type=F32)

    def inner(k, _):
        for axis, face, there in groups[2] + groups[1] + groups[0]:
            when(there, lambda axis=axis, face=face: copy_out(k, axis, face).start())

        pl.when(k == 0)(tables)

        x = x_ref[...]
        features = featured(x, charge[...])
        rows = left_rows(features)
        right[:, 0:ATOMS] = right_rows(partner_side(features, SHORT_INV)).astype(BF16)
        parts = jnp.concatenate([rows[0:8], rows[24:32], rows[40:48]], axis=0).astype(BF16)

        def own(i):
            at = slice(i * BLOCK, (i + 1) * BLOCK)
            lefts[0][at, :] = rows[:, at].T.astype(BF16)
            spread_rows(0, at, (0, 1, 2))

        pulls = []

        def pull(i):
            at = slice(i * BLOCK, (i + 1) * BLOCK)
            apart = jnp.dot(parts, incid[:, at], preferred_element_type=F32)
            apart = stiff[:, at] * (apart[0:8] + apart[8:16] + apart[16:24])
            pulls.append(jnp.concatenate(split3(apart), axis=0).astype(BF16))

        def draw(i):
            at = slice(i * BLOCK, (i + 1) * BLOCK)
            pulled = jnp.concatenate(pulls, axis=1)
            drawn = lax.dot_general(
                pulled, incid[at, :], (((1,), (1,)), ((), ())), preferred_element_type=F32
            )
            f_ref[:, at] = -(drawn[0:8] + drawn[8:16] + drawn[16:24])

        def do(work, *what):
            return functools.partial(work, *what)

        own(0)
        acc = short_sum(0, 0, zero_acc, (do(own, 1), do(pull, 0), do(pull, 1)))
        acc = short_sum(0, BLOCK, acc, (do(own, 2), do(pull, 2), do(pull, 3)))

        for item in groups[0]:
            landed(k, *item)
        acc = short_sum(0, 2 * BLOCK, acc, (do(own, 3), do(absorb, k, 1, 0), do(draw, 0), do(draw, 1)))
        acc = short_sum(0, 3 * BLOCK, acc, (do(draw, 2), do(draw, 3)))

        for axis, face, there in groups[2] + groups[1] + groups[0]:
            when(there, lambda axis=axis, face=face: copy_out(k, axis, face).wait_send())
        for item in groups[1]:
            landed(k, *item)
        acc = short_sum(1, 0, acc, (do(absorb, k, 2, 0), do(absorb, k, 2, 1), do(absorb, k, 2, 2)))

        acc = short_sum(2, 0, acc)
        acc = short_sum(2, BLOCK, acc)

        for item in groups[2]:
            landed(k, *item)
        acc = short_sum(2, 2 * BLOCK, acc, (do(absorb, k, 3, 0), do(absorb, k, 3, 1)))
        acc = short_sum(3, 0, acc)
        acc = short_sum(3, BLOCK, acc)

        force = f_ref[...] + SHORT_SCALE * gathered(acc, x)
        force = jnp.where(row < 3, force, 0.0)
        f_ref[...] = force
        v_ref[...] = v_ref[...] + (0.5 * STEP) * mass * force

        @pl.when(k < INNER - 1)
        def _():
            export(k + 1, advance())

        return 0

    lax.fori_loop(0, INNER, inner, 0)

    x = x_ref[...]
    features = featured(x, charge[...])
    right[:, 0:ATOMS] = right_rows(partner_side(features, LONG_INV)).astype(BF16)
    tiles = [(0, i, i) for i in range(OWN_TILES)]
    for group in (1, 2, 3):
        for i, (axis, face, there) in enumerate(groups[group - 1]):
            tiles += [(group, 2 * i + part, OWN_TILES + 2 * face + part) for part in range(2)]

    def spread_charge(at):
        if at < len(tiles):
            group, u, _ = tiles[at]
            spread_rows(group, slice(u * TILE, (u + 1) * TILE), (3,))

    spread_charge(0)
    acc = []
    for h in range(ATOMS // half):
        total = [jnp.zeros((8, TILE), F32) for _ in range(8)]
        for at_tile, (group, u, number) in enumerate(tiles):
            partners = lefts[group][u * TILE : (u + 1) * TILE, :]
            near = jnp.dot(partners, right[:, h * half : (h + 1) * half], preferred_element_type=F32)
            if h == 0:
                spread_charge(at_tile + 1)
            part = [jnp.zeros((8, TILE), F32) for _ in range(8)]
            for g in range(TILE // 8):
                at = slice(u * TILE + 8 * g, u * TILE + 8 * g + 8)
                xj = [spreads[group][at, c * TILE : (c + 1) * TILE] for c in range(4)]
                for t in range(2):
                    n = jnp.maximum(near[8 * g : 8 * g + 8, t * TILE : (t + 1) * TILE], 0.0) * xj[3]
                    part[4 * t] = part[4 * t] + n
                    for c in range(3):
                        part[4 * t + 1 + c] = part[4 * t + 1 + c] + n * xj[c]
            times = mult[pl.ds(number, 1), h * half : (h + 1) * half]
            for t in range(2):
                m = times[:, t * TILE : (t + 1) * TILE]
                for c in range(4):
                    total[4 * t + c] = total[4 * t + c] + m * part[4 * t + c]
        acc += total
    slow_now = LONG_SCALE * charge[...] * gathered(acc, x)
    packed_out[0:8, :] = x - start_ref[...]
    packed_out[8:16, :] = v_ref[...] + (0.5 * INNER * STEP) * mass * slow_now
    packed_out[16:24, :] = f_ref[...]
    packed_out[24:32, :] = slow_now


def finish(packed, disp_out, vel_out, fast_out, slow_out):
    disp_out[...] = packed[0:3, :]
    vel_out[...] = packed[8:11, :]
    fast_out[...] = packed[16:19, :]
    slow_out[...] = packed[24:27, :]


def on_device(pos, vel, inv_mass, charge, fast, slow, bonds, bond_k, halo, own_slot, partner_slot, count):
    vmem = pl.BlockSpec(memory_space=pltpu.VMEM)
    smem = pl.BlockSpec(memory_space=pltpu.SMEM)
    out = jax.ShapeDtypeStruct((3, ATOMS), F32)
    arrays = (
        pos, vel, inv_mass[None, :], charge[None, :], fast, slow, bonds, bond_k[None, :], halo,
        own_slot[None, :], partner_slot[None, :],
    )
    packed = pl.pallas_call(
        kernel,
        out_shape=pltpu.VMEM((32, ATOMS), F32),
        in_specs=[pl.BlockSpec(memory_space=pltpu.HBM)] * 11 + [smem],
        out_specs=vmem,
        scratch_shapes=[
            [pltpu.VMEM(a.shape, a.dtype) for a in arrays],
            pltpu.VMEM((8, ATOMS), F32),
            pltpu.VMEM((8, ATOMS), F32),
            pltpu.VMEM((8, ATOMS), F32),
            pltpu.VMEM((8, ATOMS), F32),
            pltpu.VMEM((INNER, FACES, 4, HALO), F32),
            pltpu.VMEM((INNER, FACES, 4, HALO), F32),
            [pltpu.VMEM((count, KDIM), BF16) for count in GROUPS],
            [pltpu.VMEM((count, 4 * TILE), F32) for count in GROUPS],
            pltpu.VMEM((KDIM, ATOMS + 4 * TILE), BF16),
            pltpu.VMEM((ATOMS, ATOMS), BF16),
            pltpu.VMEM((32, ATOMS), F32),
            pltpu.VMEM((8, 2 * TILE), jnp.int32),
            pltpu.SemaphoreType.DMA((INNER, FACES)),
            pltpu.SemaphoreType.DMA((INNER, FACES)),
            pltpu.SemaphoreType.DMA((11,)),
        ],
        compiler_params=pltpu.CompilerParams(
            collective_id=0, has_side_effects=True
        ),
        name="outer_step",
    )(*arrays, count[None, :])
    return pl.pallas_call(
        finish,
        out_shape=(out, out, out, out),
        in_specs=[vmem],
        out_specs=(vmem,) * 4,

        compiler_params=pltpu.CompilerParams(vmem_limit_bytes=4 * 1024 * 1024),
        name="finish",
    )(packed)


def solution(mesh):
    both = P(None, AXES)
    line = P(AXES)
    return jax.shard_map(
        on_device,
        mesh=mesh,
        in_specs=(both, both, line, line, both, both, both, line, both, line, line, line),
        out_specs=(both, both, both, both),
        check_vma=False,
    )
```
